32 devices in a mesh: ep: 8 (over z, y), dp: 4 (over x, core).
Axes of the slice: x: 2, y: 2, z: 4, core: 2. Of those that a mesh axis runs over, the one named last changes fastest.
Arguments:
- activations: float32 [16, 256, 768], P('ep', 'dp'), may hold values from -6 to 6
- out_grads: float32 [16, 256, 512], P('ep', 'dp'), may hold values from -6 to 6
- counts: int32 [16, 4], P('ep', 'dp'), may hold values from 1 to 64
- slot_weights: float32 [16, 768, 512], P('ep', None, 'dp'), may hold values from -0.21875 to 0.21875
- master: float32 [8, 768, 512], P(None, 'ep', 'dp'), may hold values from -0.21875 to 0.21875
- moment_one: float32 [8, 768, 512], P(None, 'ep', 'dp'), may hold values from -6 to 6
- moment_two: float32 [8, 768, 512], P(None, 'ep', 'dp'), may hold values from 1 to 100
- old_table: int32 [16, 1], replicated, may hold values from 0 to 7
- new_table: int32 [16, 1], replicated, may hold values from 0 to 7
Outputs:
- outputs: float32 [16, 256, 512], P('ep', 'dp')
- input_grads: float32 [16, 256, 768], P('ep', 'dp')
- new_master: float32 [8, 768, 512], P(None, 'ep', 'dp')
- new_moment_one: float32 [8, 768, 512], P(None, 'ep', 'dp')
- new_moment_two: float32 [8, 768, 512], P(None, 'ep', 'dp')
- new_slots: float32 [16, 768, 512], P('ep', None, 'dp')
The draws below stay inside these ranges and needn't reach their ends.
Inputs may be any that keep to these rules, and one draw needn't show every extreme that they name: `old_table`: every expert is named by at least one old slot. `new_table`: every expert is named by at least one new slot.
All inputs are finite; a program needn't handle non-finite values.
Results may differ from the reference program's by a relative error of at most 0.00007.
Values sent between devices are 32-bit elements; how exact they have to be, the bound alone decides.
A program may use at most 64 MiB of HBM per device.

```python
import math
import jax
import jax.numpy as jnp
from jax import lax

FF = 768
DS = 512
ROWS = 64
STEP = 100
EXPERTS = 8
SLOTS = 16
TOKS = 256
N_DP = 4


def set_ends(values, own_key, low, top_value):
    longest = values.shape.index(max(values.shape))
    spots = []
    for shift in (0, 1):
        where = [jax.random.randint(jax.random.fold_in(own_key, axis), (), 0, length) for axis, length in enumerate(values.shape)]
        where[longest] = (where[longest] + shift) % values.shape[longest]
        spots.append(tuple(where))
    return values.at[spots[0]].set(low).at[spots[1]].set(top_value)


def block_levels(key, extent, pieces, low, top_value):
    gain = 1.0
    for axis_at, parts in pieces:
        steps = jax.random.uniform(jax.random.fold_in(jax.random.fold_in(key, 6), axis_at), (parts,), jnp.float32, low / len(pieces), top_value / len(pieces))
        gain = gain * jnp.repeat(jnp.exp(steps), extent[axis_at] // parts).reshape((-1,) + (1,) * (len(extent) - 1 - axis_at))
    return gain


def choose_distinct(stream_key, rows, amount, top, lift):
    sequence = jax.random.permutation(jax.random.fold_in(stream_key, 1), amount)
    boost = sequence
    for power in range(3):
        boost = boost * boost // amount
    boost = boost * lift // amount
    tickets = jax.random.randint(jax.random.fold_in(stream_key, 2), (rows, amount), 0, 4096) + boost
    fixed_rows = jax.random.permutation(jax.random.fold_in(stream_key, 3), rows)[jnp.arange(amount) % rows]
    tickets = jnp.where(jnp.arange(rows)[:, None] == fixed_rows[None, :], 1 << 14, tickets)
    merit = tickets * amount + jnp.arange(amount)
    return lax.top_k(merit.astype(jnp.int32), top)[1].astype(jnp.int32)


def normal_values(own_key, extent, width, most, pieces=(), kind=jnp.bfloat16):
    factor_of = block_levels(own_key, extent, pieces, -0.22, 0.18) if pieces else 1.0
    array = jax.random.normal(own_key, extent, jnp.float32) * width * factor_of
    return jnp.minimum(jnp.maximum(array, -most), most).astype(kind)


def setup_inputs(seed: int = 0) -> dict:
    key_of = jax.random.split(jax.random.key(seed), 10)
    activations = normal_values(key_of[0], (SLOTS, TOKS, FF), 1.0, 6.0, ((0, 8), (1, 4)), jnp.float32)
    out_grads = normal_values(key_of[1], (SLOTS, TOKS, DS), 1.0, 6.0, ((0, 8), (1, 4)), jnp.float32)
    counts = set_ends(jax.random.randint(key_of[2], (SLOTS, N_DP), 1, ROWS + 1), jax.random.fold_in(key_of[2], 1), 1, ROWS).astype(jnp.int32)
    slot_weights = normal_values(key_of[3], (SLOTS, FF, DS), FF ** -0.5, 0.21875, ((0, 8), (2, 4)), jnp.float32)
    master = normal_values(key_of[4], (EXPERTS, FF, DS), FF ** -0.5, 0.21875, ((1, 8), (2, 4)), jnp.float32)
    moment_one = normal_values(key_of[5], (EXPERTS, FF, DS), 1.0, 6.0, ((1, 8), (2, 4)), jnp.float32)
    moment_two = jnp.clip(jnp.exp(math.log(100.0) - 4.6051702 * jax.random.uniform(key_of[6], (EXPERTS, FF, DS), jnp.float32) ** block_levels(key_of[6], (EXPERTS, FF, DS), ((1, 8), (2, 4)), -0.2, 0.2)), 1.0, 100.0)
    old_table = choose_distinct(key_of[7], SLOTS, EXPERTS, 1, 2048)
    new_table = choose_distinct(key_of[8], SLOTS, EXPERTS, 1, 1024)
    return {"activations": activations, "out_grads": out_grads, "counts": counts, "slot_weights": slot_weights, "master": master, "moment_one": moment_one, "moment_two": moment_two, "old_table": old_table, "new_table": new_table}


beta_one = 0.9
beta_two = 0.999
learn_rate = 0.02
epsilon = 1e-08
decay_rate = 0.1

def adamw(master, moment_one, moment_two, expert_grad):
    first_new = beta_one * moment_one + (1.0 - beta_one) * expert_grad
    second_new = beta_two * moment_two + (1.0 - beta_two) * expert_grad * expert_grad
    first_hat = first_new / (1.0 - beta_one ** STEP)
    second_hat = second_new / (1.0 - beta_two ** STEP)
    updated = master - learn_rate * (first_hat / (jnp.sqrt(second_hat) + epsilon) + decay_rate * master)
    return (updated, first_new, second_new)

def reference(activations, out_grads, counts, slot_weights, master, moment_one, moment_two, old_table, new_table):
    precise = lax.Precision.HIGHEST
    positions = jnp.arange(activations.shape[1], dtype=jnp.int32)
    limits = jnp.repeat(counts, ROWS, axis=1)
    live_rows = ((positions % ROWS)[None, :] < limits).astype(jnp.float32)
    masked_acts = activations * live_rows[:, :, None]
    masked_grads = out_grads * live_rows[:, :, None]
    outputs = jnp.einsum('srf,sfd->srd', masked_acts, slot_weights, precision=precise)
    input_grads = jnp.einsum('srd,sfd->srf', masked_grads, slot_weights, precision=precise)
    slot_grad = jnp.einsum('srf,srd->sfd', masked_acts, masked_grads, precision=precise)
    experts_ids = jnp.arange(EXPERTS, dtype=jnp.int32)
    old_onehot = (old_table[:, 0][None, :] == experts_ids[:, None]).astype(jnp.float32)
    expert_grad = jnp.einsum('es,sfd->efd', old_onehot, slot_grad, precision=precise)
    new_master, new_moment_one, new_moment_two = adamw(master, moment_one, moment_two, expert_grad)
    new_onehot = (new_table[:, 0][:, None] == experts_ids[None, :]).astype(jnp.float32)
    new_slots = jnp.einsum('se,efd->sfd', new_onehot, new_master, precision=precise)
    return (outputs, input_grads, new_master, new_moment_one, new_moment_two, new_slots)
```

```python
import functools

import jax
import jax.numpy as jnp
from jax import lax
from jax.experimental import pallas as pl
from jax.experimental.pallas import tpu as pltpu
from jax.sharding import PartitionSpec as P

STEP = 100
beta_one = 0.9
beta_two = 0.999
learn_rate = 0.02
epsilon = 1e-08
decay_rate = 0.1

MESH = pl.DeviceIdType.MESH


def adamw(master, moment_one, moment_two, expert_grad):
    first_new = beta_one * moment_one + (1.0 - beta_one) * expert_grad
    second_new = beta_two * moment_two + (1.0 - beta_two) * expert_grad * expert_grad
    first_hat = first_new / (1.0 - beta_one**STEP)
    second_hat = second_new / (1.0 - beta_two**STEP)
    updated = master - learn_rate * (
        first_hat / (jnp.sqrt(second_hat) + epsilon) + decay_rate * master
    )
    return (updated, first_new, second_new)


def split(x):
    high = x.astype(jnp.bfloat16)
    low = (x - high.astype(jnp.float32)).astype(jnp.bfloat16)
    return high, low


def dot3(a, b, dims):
    def one(p, q):
        return lax.dot_general(p, q, (dims, ((), ())), preferred_element_type=jnp.float32)

    return one(a[0], b[0]) + (one(a[0], b[1]) + one(a[1], b[0]))


VMEM_KIB = 52400


def piece_blocks(sides, slots, width):
    step = 128 if width % 128 == 0 else width
    found = []
    for n in range(sides):
        for s in range(slots):
            size = step if n == 0 and s == 0 else width
            found += [(n, s, low, low + size) for low in range(0, width, size)]
    return found


def kernel(nep, ndp, slots, *refs):
    old_hbm, new_hbm, counts_hbm, acts_hbm, grads_hbm, w_hbm, master_hbm, one_hbm, two_hbm = refs[:9]
    out_ref, ig_ref, nm_ref, no_ref, nt_ref = refs[9:14]
    ns_refs = refs[14:14 + slots]
    (
        acts_all, g_in, g_mask, g_send, g_cols, w_all, grad_send, arrived,
        master, one, two, pick_send, pick_recv, out_v, ig_v,
        old_ref, new_ref, counts_ref, table_sem, joined, opened,
        load_sem, store_sem,
        act_send_sem, act_recv_sem, w_send_sem, w_recv_sem, gs_sem, gr_sem,
        es_sem, er_sem, ps_sem, pr_sem,
    ) = refs[14 + slots:]
    ep = lax.axis_index("ep")
    dp = lax.axis_index("dp")
    half = ndp // 2
    sides, _, _, toks, width = acts_all.shape
    cols = w_all.shape[3]
    experts, rows, _ = master.shape
    _, chunks, _, crows, _ = grad_send.shape
    owners = nep // sides
    partner = dp + 1 - 2 * lax.rem(dp, 2)
    near = ep // owners
    quarter = ep // max(nep // 4, 1)
    outer = jnp.where((quarter == 0) | (quarter == 3), 0, 1)
    order = [lax.rem(near + outer + n, sides) for n in range(sides)]
    first = [jnp.where(side == near, 1, 0) for side in order]

    def local(src, dst, sem):
        return pltpu.make_async_copy(src, dst, sem)

    def remote(src, dst, ssem, rsem, e, d):
        return pltpu.make_async_remote_copy(
            src_ref=src, dst_ref=dst, send_sem=ssem, recv_sem=rsem,
            device_id=(e, d), device_id_type=MESH)

    tables = [local(src, dst, table_sem.at[n]) for n, (src, dst) in
              enumerate(((counts_hbm, counts_ref), (old_hbm, old_ref), (new_hbm, new_ref)))]
    load_grads = local(grads_hbm, g_in, load_sem.at[0])
    load_w = local(w_hbm, w_all.at[dp], load_sem.at[1])
    load_opt = [local(src, dst, load_sem.at[2 + n]) for n, (src, dst) in
                enumerate(((master_hbm, master), (one_hbm, one), (two_hbm, two)))]
    load_acts = [local(acts_hbm.at[:, :, pl.ds(h * width, width)], acts_all.at[h, dp], load_sem.at[5 + h])
                 for h in range(sides)]
    tables[0].start()
    for c in load_acts:
        c.start()
    load_grads.start()
    for c in tables[1:]:
        c.start()
    load_w.start()
    for c in load_opt:
        c.start()

    gate = ndp - 1
    barrier = pltpu.get_barrier_semaphore()
    for k in range(1, ndp):
        to = lax.rem(dp + k, ndp)

        @pl.when(to != gate)
        def _():
            pl.semaphore_signal(barrier, inc=1, device_id=(ep, to), device_id_type=MESH)

    @pl.when(dp != gate)
    def _():
        pl.semaphore_wait(barrier, ndp - 1)

    @pl.when(dp == gate - 1)
    def _():
        pl.semaphore_signal(joined, inc=1, device_id=(ep, gate), device_id_type=MESH)

    @pl.when(dp == gate)
    def _():
        pl.semaphore_wait(joined, 1)

        @pl.loop(1, nep)
        def _(k):
            pl.semaphore_signal(barrier, inc=1, device_id=(lax.rem(ep + k, nep), gate), device_id_type=MESH)

    def open_gate():
        @pl.when(dp == gate)
        def _():
            pl.semaphore_wait(barrier, nep - 1)
            for j in range(gate):
                pl.semaphore_signal(opened, inc=1, device_id=(ep, j), device_id_type=MESH)

    def pass_gate():
        @pl.when(dp != gate)
        def _():
            pl.semaphore_wait(opened, 1)

    def grad_copy(k, s):
        to = lax.rem(dp - k + ndp, ndp)
        return remote(g_send.at[to, s], g_cols.at[dp, s], gs_sem.at[k - 1, s], gr_sem.at[k - 1, s], ep, to)

    def grad_arrival(k, s):
        came = g_cols.at[lax.rem(dp + k, ndp), s]
        return remote(came, came, gs_sem.at[k - 1, s], gr_sem.at[k - 1, s], ep, partner)

    def block_copy(view, k, ssem, rsem):
        own = view(dp)
        to = partner if k == 0 else lax.rem(dp - 2 * k + ndp, ndp)
        return remote(own, own, ssem(k), rsem(k), ep, to)

    def block_arrival(view, k, ssem, rsem):
        if k == 0:
            came = view(partner)
        elif k < half:
            came = view(lax.rem(dp + 2 * k, ndp))
        else:
            came = view(lax.rem(partner + 2 * (k - half + 1), ndp))
        return remote(came, came, ssem(k), rsem(k), ep, partner)

    def block_relay(view, k, ssem, rsem):
        block = view(lax.rem(dp + 2 * k, ndp))
        return remote(block, block, ssem(half - 1 + k), rsem(half - 1 + k), ep, partner)

    def acts_kit(b):
        n, s, low, high = blocks[b]
        return (lambda i: acts_all.at[order[n], i, s, :, pl.ds(low, high - low)],
                lambda k: act_send_sem.at[k, b], lambda k: act_recv_sem.at[k, b])

    def w_kit(s):
        return (lambda i: w_all.at[i, s], lambda k: w_send_sem.at[k, s], lambda k: w_recv_sem.at[k, s])

    def send_block(view, ssem, rsem):
        for k in range(half - 1, -1, -1):
            block_copy(view, k, ssem, rsem).start()

    def relay_block(view, ssem, rsem):
        for k in range(1, half):
            block_arrival(view, k, ssem, rsem).wait_recv()
            block_relay(view, k, ssem, rsem).start()

    def finish_block(view, ssem, rsem):
        block_arrival(view, 0, ssem, rsem).wait_recv()
        for k in range(half, ndp - 1):
            block_arrival(view, k, ssem, rsem).wait_recv()

    pieces = [(n, s) for n in range(sides) for s in range(slots)]
    blocks = piece_blocks(sides, slots, width)

    for c in load_acts:
        c.wait()
    send_block(*acts_kit(0))
    tables[0].wait()
    load_grads.wait()
    for s in range(slots):
        live = (lax.broadcasted_iota(jnp.int32, (toks, 1), 0) < counts_ref[s]).astype(jnp.float32)
        masked = g_in[s] * live
        g_mask[s] = masked
        for j in range(ndp):
            g_send[j, s] = masked[:, j * cols:(j + 1) * cols]
        g_cols[dp, s] = g_send[dp, s]
        for k in range(ndp - 1, 0, -1):
            grad_copy(k, s).start()
        if s == 0:
            for b, (n, t, _, _) in enumerate(blocks):
                if b and (n, t) == pieces[0]:
                    send_block(*acts_kit(b))
    for b, (n, s, _, _) in enumerate(blocks):
        if (n, s) != pieces[0]:
            send_block(*acts_kit(b))
    load_w.wait()
    for s in range(slots):
        send_block(*w_kit(s))

    def send_grad(n, s, c):
        base = order[n] * owners

        @pl.loop(first[n], owners)
        def _(k):
            to = base + lax.rem(ep + k, owners)
            remote(grad_send.at[s, c, to], arrived.at[s, c, ep], es_sem.at[s, c], er_sem.at[s, c], to, dp).start()

    def send_some(n, s, start, stop):
        base = order[n] * owners

        @pl.loop(start, stop)
        def _(i):
            to = base + i

            @pl.when(to != ep)
            def _():
                for c in range(chunks):
                    remote(grad_send.at[s, c, to], arrived.at[s, c, ep], es_sem.at[s, c], er_sem.at[s, c], to, dp).start()

    rights = {}
    for b, (n, s, low, high) in enumerate(blocks):
        relay_block(*acts_kit(b))
        if b == 0:
            open_gate()
        if s not in rights:
            for k in range(1, ndp):
                grad_arrival(k, s).wait_recv()
            rights[s] = split(g_cols[:, s].reshape(ndp * toks, cols))
        finish_block(*acts_kit(b))
        left = split(acts_all[order[n], :, s, :, low:high].reshape(ndp * toks, high - low))
        grad = dot3(left, rights[s], ((0,), (0,)))
        base = order[n] * owners
        for i in range(owners):
            for c in range(chunks):
                at = i * rows + c * crows
                start, stop = max(at, low), min(at + crows, high)
                if start < stop:
                    grad_send[s, c, base + i, start - at:stop - at] = grad[start - low:stop - low]
        if b == 0:
            pass_gate()
        if (n, s) == pieces[0]:
            send_some(n, s, low // rows, high // rows)
        else:
            send_grad(n, s, 0)
    for c in range(1, chunks):
        for n, s in pieces[1:]:
            send_grad(n, s, c)
    for s in range(slots):
        for c in range(chunks):
            arrived[s, c, ep] = grad_send[s, c, ep]

    for c in tables[1:] + load_opt:
        c.wait()

    direct = rows % 8 == 0

    def landing(s, c, i):
        if direct:
            return ns_refs[s].at[pl.ds(pl.multiple_of(i * rows + c * crows, 8), crows)]
        return pick_recv.at[s, i]

    own_stores = []
    for c in range(chunks):
        for s in range(slots):
            came = arrived.at[s, c, pl.ds(0, nep - 1)]
            remote(came, came, es_sem.at[s, c], er_sem.at[s, c], ep, partner).wait_recv()
        span = slice(c * crows, (c + 1) * crows)

        @pl.loop(0, experts)
        def _(e):
            total = jnp.zeros((crows, cols), jnp.float32)
            for i in range(nep):
                for s in range(slots):
                    held = jnp.where(old_ref[i * slots + s] == e, 1.0, 0.0)
                    total = total + held * arrived[s, c, i]
            master[e, span], one[e, span], two[e, span] = adamw(
                master[e, span], one[e, span], two[e, span], total)

        def send_pick(to):
            for s in range(slots):
                pick_send[s, c, to] = master[new_ref[to * slots + s], span]
            for s in range(slots):
                remote(pick_send.at[s, c, to], landing(s, c, ep), ps_sem.at[s, c], pr_sem.at[s, c], to, dp).start()

        for n in range(sides):
            base = order[n] * owners

            @pl.loop(first[n], owners)
            def _(k):
                send_pick(base + lax.rem(ep + k, owners))

        for s in range(slots):
            pick_send[s, c, ep] = master[new_ref[ep * slots + s], span]
            own_stores.append(local(pick_send.at[s, c, ep], landing(s, c, ep), store_sem.at[5 + s, c]))
            own_stores[-1].start()

    stores = [local(src, dst, store_sem.at[n, 0]) for n, (src, dst) in
              enumerate(((master, nm_ref), (one, no_ref), (two, nt_ref)))]
    for c in stores:
        c.start()

    for s in range(slots):
        relay_block(*w_kit(s))
    last = []
    for s in range(slots):
        finish_block(*w_kit(s))
        live = (lax.broadcasted_iota(jnp.int32, (toks, 1), 0) < counts_ref[s]).astype(jnp.float32)
        acts = [split(acts_all[h, dp, s] * live) for h in range(sides)]
        back = [jnp.zeros((toks, width), jnp.float32) for h in range(sides)]
        for j in range(ndp):
            at = slice(j * cols, (j + 1) * cols)
            grads = split(g_mask[s, :, at])
            total = jnp.zeros((toks, cols), jnp.float32)
            for h in range(sides):
                weights = split(w_all[j, s, h * width:(h + 1) * width])
                total = total + dot3(acts[h], weights, ((1,), (0,)))
                back[h] = back[h] + dot3(grads, weights, ((1,), (1,)))
            out_v[s, :, at] = total
        for h in range(sides):
            ig_v[s, :, h * width:(h + 1) * width] = back[h]
    last = [local(out_v, out_ref, store_sem.at[3, 0]), local(ig_v, ig_ref, store_sem.at[4, 0])]
    for c in last:
        c.start()

    for s in range(slots):
        for k in range(1, ndp):
            grad_copy(k, s).wait_send()
    for kit in [acts_kit(b) for b in range(len(blocks))] + [w_kit(s) for s in range(slots)]:
        for k in range(half):
            block_copy(kit[0], k, *kit[1:]).wait_send()
        for k in range(1, half):
            block_relay(kit[0], k, *kit[1:]).wait_send()
    for s in range(slots):
        for c in range(chunks):
            gone = grad_send.at[s, c, pl.ds(0, nep - 1)]
            remote(gone, gone, es_sem.at[s, c], er_sem.at[s, c], ep, partner).wait_send()
            gone = pick_send.at[s, c, pl.ds(0, nep - 1)]
            remote(gone, gone, ps_sem.at[s, c], pr_sem.at[s, c], ep, partner).wait_send()
    for c in own_stores + stores + last:
        c.wait()
    for s in range(slots):
        for c in range(chunks):
            if direct:
                came = ns_refs[s].at[pl.ds(0, (nep - 1) * crows)]
            else:
                came = pick_recv.at[s, pl.ds(0, nep - 1)]
            remote(came, came, ps_sem.at[s, c], pr_sem.at[s, c], ep, partner).wait_recv()
    if not direct:
        for s in range(slots):
            for i in range(nep):
                w_all[0, s, i * rows:(i + 1) * rows] = pick_recv[s, i]
            done = local(w_all.at[0, s], ns_refs[s], store_sem.at[0, 0])
            done.start()
            done.wait()


def write_out(slots, *refs):
    ins, outs, sems = refs[:5 + slots], refs[5 + slots:-1], refs[-1]
    parts = list(outs[:5]) + [outs[5].at[n] for n in range(slots)]
    copies = [pltpu.make_async_copy(src, dst, sems.at[n]) for n, (src, dst) in enumerate(zip(ins, parts))]
    for c in copies:
        c.start()
    for c in copies:
        c.wait()


def local_step(nep, ndp, activations, out_grads, counts, slot_weights, master, moment_one, moment_two, old_table, new_table):
    f32 = jnp.float32
    slots, toks, ff = activations.shape
    ds = out_grads.shape[2]
    cols = slot_weights.shape[2]
    experts, rows, _ = master.shape
    direct = rows % 8 == 0
    sides = 2
    chunks = 2 if rows % 16 == 0 else 1
    blocks = len(piece_blocks(sides, slots, ff // sides))
    parted = (slots, chunks, nep, rows // chunks, cols)
    hbm = pl.BlockSpec(memory_space=pl.ANY)
    dma = pltpu.SemaphoreType.DMA
    shapes = [
        jax.ShapeDtypeStruct(x.shape, f32)
        for x in (out_grads, activations, master, moment_one, moment_two, slot_weights)
    ]
    results = pl.pallas_call(
        functools.partial(kernel, nep, ndp, slots),
        out_shape=shapes[:5] + [jax.ShapeDtypeStruct((ff, cols), f32)] * slots,
        in_specs=[hbm] * 9,
        out_specs=[hbm] * (5 + slots),
        scratch_shapes=[
            pltpu.VMEM((sides, ndp, slots, toks, ff // sides), f32),
            pltpu.VMEM((slots, toks, ds), f32),
            pltpu.VMEM((slots, toks, ds), f32),
            pltpu.VMEM((ndp, slots, toks, cols), f32),
            pltpu.VMEM((ndp, slots, toks, cols), f32),
            pltpu.VMEM((ndp, slots, ff, cols), f32),
            pltpu.VMEM(parted, f32),
            pltpu.VMEM(parted, f32),
            pltpu.VMEM((experts, rows, cols), f32),
            pltpu.VMEM((experts, rows, cols), f32),
            pltpu.VMEM((experts, rows, cols), f32),
            pltpu.VMEM(parted, f32),
            pltpu.VMEM((1, 1, 8, 128) if direct else (slots, nep, rows, cols), f32),
            pltpu.VMEM((slots, toks, ds), f32),
            pltpu.VMEM((slots, toks, ff), f32),
            pltpu.SMEM((nep * slots,), jnp.int32),
            pltpu.SMEM((nep * slots,), jnp.int32),
            pltpu.SMEM((slots,), jnp.int32),
            dma((3,)),
            pltpu.SemaphoreType.REGULAR,
            pltpu.SemaphoreType.REGULAR,
            dma((5 + sides,)),
            dma((5 + slots, chunks)),
            dma((ndp - 1, blocks)),
            dma((ndp - 1, blocks)),
            dma((ndp - 1, slots)),
            dma((ndp - 1, slots)),
            dma((ndp - 1, slots)),
            dma((ndp - 1, slots)),
            dma((slots, chunks)),
            dma((slots, chunks)),
            dma((slots, chunks)),
            dma((slots, chunks)),
        ],
        compiler_params=pltpu.CompilerParams(
            collective_id=0, has_side_effects=True, vmem_limit_bytes=VMEM_KIB * 1024
        ),
        name="step",
    )(*[pltpu.with_memory_space_constraint(x, pltpu.HBM) for x in (
        old_table.reshape(-1), new_table.reshape(-1), counts.reshape(-1),
        activations, out_grads, slot_weights, master, moment_one, moment_two)])
    return pl.pallas_call(
        functools.partial(write_out, slots),
        out_shape=shapes,
        in_specs=[hbm] * (5 + slots),
        out_specs=[hbm] * 6,
        scratch_shapes=[dma((5 + slots,))],
        compiler_params=pltpu.CompilerParams(vmem_limit_bytes=1024 * 1024),
        name="write_out",
    )(*results)


def solution(mesh):
    in_specs = (
        P("ep", "dp", None),
        P("ep", "dp", None),
        P("ep", "dp"),
        P("ep", None, "dp"),
        P(None, "ep", "dp"),
        P(None, "ep", "dp"),
        P(None, "ep", "dp"),
        P(),
        P(),
    )
    out_specs = (
        P("ep", "dp", None),
        P("ep", "dp", None),
        P(None, "ep", "dp"),
        P(None, "ep", "dp"),
        P(None, "ep", "dp"),
        P("ep", None, "dp"),
    )
    step = functools.partial(local_step, mesh.shape["ep"], mesh.shape["dp"])
    return jax.shard_map(step, mesh=mesh, in_specs=in_specs, out_specs=out_specs, check_vma=False)
```

```python
import functools

import jax
import jax.numpy as jnp
from jax import lax
from jax.experimental import pallas as pl
from jax.experimental.pallas import tpu as pltpu
from jax.sharding import PartitionSpec as P

STEP = 100
beta_one = 0.9
beta_two = 0.999
learn_rate = 0.02
epsilon = 1e-08
decay_rate = 0.1

MESH = pl.DeviceIdType.MESH


def adamw(master, moment_one, moment_two, expert_grad):
    first_new = beta_one * moment_one + (1.0 - beta_one) * expert_grad
    second_new = beta_two * moment_two + (1.0 - beta_two) * expert_grad * expert_grad
    first_hat = first_new / (1.0 - beta_one**STEP)
    second_hat = second_new / (1.0 - beta_two**STEP)
    updated = master - learn_rate * (
        first_hat / (jnp.sqrt(second_hat) + epsilon) + decay_rate * master
    )
    return (updated, first_new, second_new)


def split(x):
    high = x.astype(jnp.bfloat16)
    low = (x - high.astype(jnp.float32)).astype(jnp.bfloat16)
    return high, low


def dot3(a, b, dims):
    def one(p, q):
        return lax.dot_general(p, q, (dims, ((), ())), preferred_element_type=jnp.float32)

    return one(a[0], b[0]) + (one(a[0], b[1]) + one(a[1], b[0]))


VMEM_KIB = 52400


def piece_blocks(sides, slots, width):
    step = 128 if width % 128 == 0 else width
    found = []
    for n in range(sides):
        for s in range(slots):
            size = step if n == 0 and s == 0 else width
            found += [(n, s, low, low + size) for low in range(0, width, size)]
    return found


def kernel(nep, ndp, slots, *refs):
    old_hbm, new_hbm, counts_hbm, acts_hbm, grads_hbm, w_hbm, master_hbm, one_hbm, two_hbm = refs[:9]
    out_ref, ig_ref, nm_ref, no_ref, nt_ref = refs[9:14]
    ns_refs = refs[14:14 + slots]
    (
        acts_all, g_in, g_mask, g_send, g_cols, w_all, grad_send, arrived,
        master, one, two, pick_send, pick_recv, out_v, ig_v,
        old_ref, new_ref, counts_ref, table_sem, joined, opened,
        load_sem, store_sem,
        act_send_sem, act_recv_sem, w_send_sem, w_recv_sem, gs_sem, gr_sem,
        es_sem, er_sem, ps_sem, pr_sem,
    ) = refs[14 + slots:]
    ep = lax.axis_index("ep")
    dp = lax.axis_index("dp")
    half = ndp // 2
    sides, _, _, toks, width = acts_all.shape
    cols = w_all.shape[3]
    experts, rows, _ = master.shape
    _, chunks, _, crows, _ = grad_send.shape
    owners = nep // sides
    partner = dp + 1 - 2 * lax.rem(dp, 2)
    near = ep // owners
    quarter = ep // max(nep // 4, 1)
    outer = jnp.where((quarter == 0) | (quarter == 3), 0, 1)
    order = [lax.rem(near + outer + n, sides) for n in range(sides)]
    first = [jnp.where(side == near, 1, 0) for side in order]
    away = [lax.rem(near + 1 + n, sides) for n in range(sides)]
    skip = [0] * (sides - 1) + [1]

    def local(src, dst, sem):
        return pltpu.make_async_copy(src, dst, sem)

    def remote(src, dst, ssem, rsem, e, d):
        return pltpu.make_async_remote_copy(
            src_ref=src, dst_ref=dst, send_sem=ssem, recv_sem=rsem,
            device_id=(e, d), device_id_type=MESH)

    tables = [local(src, dst, table_sem.at[n]) for n, (src, dst) in
              enumerate(((counts_hbm, counts_ref), (old_hbm, old_ref), (new_hbm, new_ref)))]
    load_grads = local(grads_hbm, g_in, load_sem.at[0])
    load_w = local(w_hbm, w_all.at[dp], load_sem.at[1])
    load_opt = [local(src, dst, load_sem.at[2 + n]) for n, (src, dst) in
                enumerate(((master_hbm, master), (one_hbm, one), (two_hbm, two)))]
    load_acts = [local(acts_hbm.at[:, :, pl.ds(h * width, width)], acts_all.at[h, dp], load_sem.at[5 + h])
                 for h in range(sides)]
    tables[0].start()
    for c in load_acts:
        c.start()
    load_grads.start()
    for c in tables[1:]:
        c.start()
    load_w.start()
    for c in load_opt:
        c.start()

    gate = ndp - 1
    barrier = pltpu.get_barrier_semaphore()
    for k in range(1, ndp):
        to = lax.rem(dp + k, ndp)

        @pl.when(to != gate)
        def _():
            pl.semaphore_signal(barrier, inc=1, device_id=(ep, to), device_id_type=MESH)

    @pl.when(dp != gate)
    def _():
        pl.semaphore_wait(barrier, ndp - 1)

    @pl.when(dp == gate - 1)
    def _():
        pl.semaphore_signal(joined, inc=1, device_id=(ep, gate), device_id_type=MESH)

    @pl.when(dp == gate)
    def _():
        pl.semaphore_wait(joined, 1)

        @pl.loop(1, nep)
        def _(k):
            pl.semaphore_signal(barrier, inc=1, device_id=(lax.rem(ep + k, nep), gate), device_id_type=MESH)

    def open_gate():
        @pl.when(dp == gate)
        def _():
            pl.semaphore_wait(barrier, nep - 1)
            for j in range(gate):
                pl.semaphore_signal(opened, inc=1, device_id=(ep, j), device_id_type=MESH)

    def pass_gate():
        @pl.when(dp != gate)
        def _():
            pl.semaphore_wait(opened, 1)

    def grad_copy(k, s):
        to = lax.rem(dp - k + ndp, ndp)
        return remote(g_send.at[to, s], g_cols.at[dp, s], gs_sem.at[k - 1, s], gr_sem.at[k - 1, s], ep, to)

    def grad_arrival(k, s):
        came = g_cols.at[lax.rem(dp + k, ndp), s]
        return remote(came, came, gs_sem.at[k - 1, s], gr_sem.at[k - 1, s], ep, partner)

    def block_copy(view, k, ssem, rsem):
        own = view(dp)
        to = partner if k == 0 else lax.rem(dp - 2 * k + ndp, ndp)
        return remote(own, own, ssem(k), rsem(k), ep, to)

    def block_arrival(view, k, ssem, rsem):
        if k == 0:
            came = view(partner)
        elif k < half:
            came = view(lax.rem(dp + 2 * k, ndp))
        else:
            came = view(lax.rem(partner + 2 * (k - half + 1), ndp))
        return remote(came, came, ssem(k), rsem(k), ep, partner)

    def block_relay(view, k, ssem, rsem):
        block = view(lax.rem(dp + 2 * k, ndp))
        return remote(block, block, ssem(half - 1 + k), rsem(half - 1 + k), ep, partner)

    def acts_kit(b):
        n, s, low, high = blocks[b]
        return (lambda i: acts_all.at[away[n], i, s, :, pl.ds(low, high - low)],
                lambda k: act_send_sem.at[k, b], lambda k: act_recv_sem.at[k, b])

    def w_kit(s):
        return (lambda i: w_all.at[i, s], lambda k: w_send_sem.at[k, s], lambda k: w_recv_sem.at[k, s])

    def send_block(view, ssem, rsem):
        for k in range(half - 1, -1, -1):
            block_copy(view, k, ssem, rsem).start()

    def relay_block(view, ssem, rsem):
        for k in range(1, half):
            block_arrival(view, k, ssem, rsem).wait_recv()
            block_relay(view, k, ssem, rsem).start()

    def finish_block(view, ssem, rsem):
        block_arrival(view, 0, ssem, rsem).wait_recv()
        for k in range(half, ndp - 1):
            block_arrival(view, k, ssem, rsem).wait_recv()

    pieces = [(n, s) for n in range(sides) for s in range(slots)]
    blocks = piece_blocks(sides, slots, width)

    for c in load_acts:
        c.wait()
    send_block(*acts_kit(0))
    tables[0].wait()
    load_grads.wait()
    for s in range(slots):
        live = (lax.broadcasted_iota(jnp.int32, (toks, 1), 0) < counts_ref[s]).astype(jnp.float32)
        masked = g_in[s] * live
        g_mask[s] = masked
        for j in range(ndp):
            g_send[j, s] = masked[:, j * cols:(j + 1) * cols]
        g_cols[dp, s] = g_send[dp, s]
        for k in range(ndp - 1, 0, -1):
            grad_copy(k, s).start()
        if s == 0:
            for b, (n, t, _, _) in enumerate(blocks):
                if b and (n, t) == pieces[0]:
                    send_block(*acts_kit(b))
    for b, (n, s, _, _) in enumerate(blocks):
        if (n, s) != pieces[0]:
            send_block(*acts_kit(b))
    load_w.wait()
    for s in range(slots):
        send_block(*w_kit(s))

    def send_grad(n, s, c):
        base = away[n] * owners

        @pl.loop(skip[n], owners)
        def _(k):
            to = base + lax.rem(ep + k, owners)
            remote(grad_send.at[s, c, to], arrived.at[s, c, ep], es_sem.at[s, c], er_sem.at[s, c], to, dp).start()

    def send_some(n, s, start, stop):
        base = away[n] * owners

        @pl.loop(start, stop)
        def _(i):
            to = base + i

            @pl.when(to != ep)
            def _():
                for c in range(chunks):
                    remote(grad_send.at[s, c, to], arrived.at[s, c, ep], es_sem.at[s, c], er_sem.at[s, c], to, dp).start()

    rights = {}
    for b, (n, s, low, high) in enumerate(blocks):
        relay_block(*acts_kit(b))
        if b == 0:
            open_gate()
        if s not in rights:
            for k in range(1, ndp):
                grad_arrival(k, s).wait_recv()
            rights[s] = split(g_cols[:, s].reshape(ndp * toks, cols))
        finish_block(*acts_kit(b))
        left = split(acts_all[away[n], :, s, :, low:high].reshape(ndp * toks, high - low))
        grad = dot3(left, rights[s], ((0,), (0,)))
        base = away[n] * owners
        for i in range(owners):
            for c in range(chunks):
                at = i * rows + c * crows
                start, stop = max(at, low), min(at + crows, high)
                if start < stop:
                    grad_send[s, c, base + i, start - at:stop - at] = grad[start - low:stop - low]
        if b == 0:
            pass_gate()
        if (n, s) == pieces[0]:
            send_some(n, s, low // rows, high // rows)
        else:
            send_grad(n, s, 0)
    for c in range(1, chunks):
        for n, s in pieces[1:]:
            send_grad(n, s, c)
    for s in range(slots):
        for c in range(chunks):
            arrived[s, c, ep] = grad_send[s, c, ep]

    for c in tables[1:] + load_opt:
        c.wait()

    direct = rows % 8 == 0

    def landing(s, c, i):
        if direct:
            return ns_refs[s].at[pl.ds(pl.multiple_of(i * rows + c * crows, 8), crows)]
        return pick_recv.at[s, i]

    own_stores = []
    for c in range(chunks):
        for s in range(slots):
            came = arrived.at[s, c, pl.ds(0, nep - 1)]
            remote(came, came, es_sem.at[s, c], er_sem.at[s, c], ep, partner).wait_recv()
        span = slice(c * crows, (c + 1) * crows)

        @pl.loop(0, experts)
        def _(e):
            total = jnp.zeros((crows, cols), jnp.float32)
            for i in range(nep):
                for s in range(slots):
                    held = jnp.where(old_ref[i * slots + s] == e, 1.0, 0.0)
                    total = total + held * arrived[s, c, i]
            master[e, span], one[e, span], two[e, span] = adamw(
                master[e, span], one[e, span], two[e, span], total)

        def send_pick(to):
            for s in range(slots):
                pick_send[s, c, to] = master[new_ref[to * slots + s], span]
            for s in range(slots):
                remote(pick_send.at[s, c, to], landing(s, c, ep), ps_sem.at[s, c], pr_sem.at[s, c], to, dp).start()

        for n in range(sides):
            base = order[n] * owners

            @pl.loop(first[n], owners)
            def _(k):
                send_pick(base + lax.rem(ep + k, owners))

        for s in range(slots):
            pick_send[s, c, ep] = master[new_ref[ep * slots + s], span]
            own_stores.append(local(pick_send.at[s, c, ep], landing(s, c, ep), store_sem.at[5 + s, c]))
            own_stores[-1].start()

    stores = [local(src, dst, store_sem.at[n, 0]) for n, (src, dst) in
              enumerate(((master, nm_ref), (one, no_ref), (two, nt_ref)))]
    for c in stores:
        c.start()

    for s in range(slots):
        relay_block(*w_kit(s))
    last = []
    for s in range(slots):
        finish_block(*w_kit(s))
        live = (lax.broadcasted_iota(jnp.int32, (toks, 1), 0) < counts_ref[s]).astype(jnp.float32)
        acts = [split(acts_all[h, dp, s] * live) for h in range(sides)]
        back = [jnp.zeros((toks, width), jnp.float32) for h in range(sides)]
        for j in range(ndp):
            at = slice(j * cols, (j + 1) * cols)
            grads = split(g_mask[s, :, at])
            total = jnp.zeros((toks, cols), jnp.float32)
            for h in range(sides):
                weights = split(w_all[j, s, h * width:(h + 1) * width])
                total = total + dot3(acts[h], weights, ((1,), (0,)))
                back[h] = back[h] + dot3(grads, weights, ((1,), (1,)))
            out_v[s, :, at] = total
        for h in range(sides):
            ig_v[s, :, h * width:(h + 1) * width] = back[h]
    last = [local(out_v, out_ref, store_sem.at[3, 0]), local(ig_v, ig_ref, store_sem.at[4, 0])]
    for c in last:
        c.start()

    for s in range(slots):
        for k in range(1, ndp):
            grad_copy(k, s).wait_send()
    for kit in [acts_kit(b) for b in range(len(blocks))] + [w_kit(s) for s in range(slots)]:
        for k in range(half):
            block_copy(kit[0], k, *kit[1:]).wait_send()
        for k in range(1, half):
            block_relay(kit[0], k, *kit[1:]).wait_send()
    for s in range(slots):
        for c in range(chunks):
            gone = grad_send.at[s, c, pl.ds(0, nep - 1)]
            remote(gone, gone, es_sem.at[s, c], er_sem.at[s, c], ep, partner).wait_send()
            gone = pick_send.at[s, c, pl.ds(0, nep - 1)]
            remote(gone, gone, ps_sem.at[s, c], pr_sem.at[s, c], ep, partner).wait_send()
    for c in own_stores + stores + last:
        c.wait()
    for s in range(slots):
        for c in range(chunks):
            if direct:
                came = ns_refs[s].at[pl.ds(0, (nep - 1) * crows)]
            else:
                came = pick_recv.at[s, pl.ds(0, nep - 1)]
            remote(came, came, ps_sem.at[s, c], pr_sem.at[s, c], ep, partner).wait_recv()
    if not direct:
        for s in range(slots):
            for i in range(nep):
                w_all[0, s, i * rows:(i + 1) * rows] = pick_recv[s, i]
            done = local(w_all.at[0, s], ns_refs[s], store_sem.at[0, 0])
            done.start()
            done.wait()


def write_out(slots, *refs):
    ins, outs, sems = refs[:5 + slots], refs[5 + slots:-1], refs[-1]
    parts = list(outs[:5]) + [outs[5].at[n] for n in range(slots)]
    copies = [pltpu.make_async_copy(src, dst, sems.at[n]) for n, (src, dst) in enumerate(zip(ins, parts))]
    for c in copies:
        c.start()
    for c in copies:
        c.wait()


def local_step(nep, ndp, activations, out_grads, counts, slot_weights, master, moment_one, moment_two, old_table, new_table):
    f32 = jnp.float32
    slots, toks, ff = activations.shape
    ds = out_grads.shape[2]
    cols = slot_weights.shape[2]
    experts, rows, _ = master.shape
    direct = rows % 8 == 0
    sides = 2
    chunks = 2 if rows % 16 == 0 else 1
    blocks = len(piece_blocks(sides, slots, ff // sides))
    parted = (slots, chunks, nep, rows // chunks, cols)
    hbm = pl.BlockSpec(memory_space=pl.ANY)
    dma = pltpu.SemaphoreType.DMA
    shapes = [
        jax.ShapeDtypeStruct(x.shape, f32)
        for x in (out_grads, activations, master, moment_one, moment_two, slot_weights)
    ]
    results = pl.pallas_call(
        functools.partial(kernel, nep, ndp, slots),
        out_shape=shapes[:5] + [jax.ShapeDtypeStruct((ff, cols), f32)] * slots,
        in_specs=[hbm] * 9,
        out_specs=[hbm] * (5 + slots),
        scratch_shapes=[
            pltpu.VMEM((sides, ndp, slots, toks, ff // sides), f32),
            pltpu.VMEM((slots, toks, ds), f32),
            pltpu.VMEM((slots, toks, ds), f32),
            pltpu.VMEM((ndp, slots, toks, cols), f32),
            pltpu.VMEM((ndp, slots, toks, cols), f32),
            pltpu.VMEM((ndp, slots, ff, cols), f32),
            pltpu.VMEM(parted, f32),
            pltpu.VMEM(parted, f32),
            pltpu.VMEM((experts, rows, cols), f32),
            pltpu.VMEM((experts, rows, cols), f32),
            pltpu.VMEM((experts, rows, cols), f32),
            pltpu.VMEM(parted, f32),
            pltpu.VMEM((1, 1, 8, 128) if direct else (slots, nep, rows, cols), f32),
            pltpu.VMEM((slots, toks, ds), f32),
            pltpu.VMEM((slots, toks, ff), f32),
            pltpu.SMEM((nep * slots,), jnp.int32),
            pltpu.SMEM((nep * slots,), jnp.int32),
            pltpu.SMEM((slots,), jnp.int32),
            dma((3,)),
            pltpu.SemaphoreType.REGULAR,
            pltpu.SemaphoreType.REGULAR,
            dma((5 + sides,)),
            dma((5 + slots, chunks)),
            dma((ndp - 1, blocks)),
            dma((ndp - 1, blocks)),
            dma((ndp - 1, slots)),
            dma((ndp - 1, slots)),
            dma((ndp - 1, slots)),
            dma((ndp - 1, slots)),
            dma((slots, chunks)),
            dma((slots, chunks)),
            dma((slots, chunks)),
            dma((slots, chunks)),
        ],
        compiler_params=pltpu.CompilerParams(
            collective_id=0, has_side_effects=True, vmem_limit_bytes=VMEM_KIB * 1024
        ),
        name="step",
    )(*[pltpu.with_memory_space_constraint(x, pltpu.HBM) for x in (
        old_table.reshape(-1), new_table.reshape(-1), counts.reshape(-1),
        activations, out_grads, slot_weights, master, moment_one, moment_two)])
    return pl.pallas_call(
        functools.partial(write_out, slots),
        out_shape=shapes,
        in_specs=[hbm] * (5 + slots),
        out_specs=[hbm] * 6,
        scratch_shapes=[dma((5 + slots,))],
        compiler_params=pltpu.CompilerParams(vmem_limit_bytes=1024 * 1024),
        name="write_out",
    )(*results)


def solution(mesh):
    in_specs = (
        P("ep", "dp", None),
        P("ep", "dp", None),
        P("ep", "dp"),
        P("ep", None, "dp"),
        P(None, "ep", "dp"),
        P(None, "ep", "dp"),
        P(None, "ep", "dp"),
        P(),
        P(),
    )
    out_specs = (
        P("ep", "dp", None),
        P("ep", "dp", None),
        P(None, "ep", "dp"),
        P(None, "ep", "dp"),
        P(None, "ep", "dp"),
        P("ep", None, "dp"),
    )
    step = functools.partial(local_step, mesh.shape["ep"], mesh.shape["dp"])
    return jax.shard_map(step, mesh=mesh, in_specs=in_specs, out_specs=out_specs, check_vma=False)
```

```python
import functools

import jax
import jax.numpy as jnp
from jax import lax
from jax.experimental import pallas as pl
from jax.experimental.pallas import tpu as pltpu
from jax.sharding import PartitionSpec as P

STEP = 100
beta_one = 0.9
beta_two = 0.999
learn_rate = 0.02
epsilon = 1e-08
decay_rate = 0.1

MESH = pl.DeviceIdType.MESH


def adamw(master, moment_one, moment_two, expert_grad):
    first_new = beta_one * moment_one + (1.0 - beta_one) * expert_grad
    second_new = beta_two * moment_two + (1.0 - beta_two) * expert_grad * expert_grad
    first_hat = first_new / (1.0 - beta_one**STEP)
    second_hat = second_new / (1.0 - beta_two**STEP)
    updated = master - learn_rate * (
        first_hat / (jnp.sqrt(second_hat) + epsilon) + decay_rate * master
    )
    return (updated, first_new, second_new)


def split(x):
    high = x.astype(jnp.bfloat16)
    low = (x - high.astype(jnp.float32)).astype(jnp.bfloat16)
    return high, low


def dot3(a, b, dims):
    def one(p, q):
        return lax.dot_general(p, q, (dims, ((), ())), preferred_element_type=jnp.float32)

    return one(a[0], b[0]) + (one(a[0], b[1]) + one(a[1], b[0]))


VMEM_KIB = 52400


def piece_blocks(sides, slots, width):
    step = 128 if width % 128 == 0 else width
    found = []
    for n in range(sides):
        for s in range(slots):
            size = step if n == 0 and s == 0 else width
            found += [(n, s, low, low + size) for low in range(0, width, size)]
    return found


def kernel(nep, ndp, slots, *refs):
    old_hbm, new_hbm, counts_hbm, acts_hbm, grads_hbm, w_hbm, master_hbm, one_hbm, two_hbm = refs[:9]
    out_ref, ig_ref, nm_ref, no_ref, nt_ref = refs[9:14]
    ns_refs = refs[14:14 + slots]
    (
        acts_all, g_in, g_mask, g_send, g_cols, w_all, grad_send, arrived,
        master, one, two, pick_send, pick_recv, out_v, ig_v,
        old_ref, new_ref, counts_ref, table_sem, joined, opened,
        load_sem, store_sem,
        act_send_sem, act_recv_sem, w_send_sem, w_recv_sem, gs_sem, gr_sem,
        es_sem, er_sem, ps_sem, pr_sem,
    ) = refs[14 + slots:]
    ep = lax.axis_index("ep")
    dp = lax.axis_index("dp")
    half = ndp // 2
    sides, _, _, toks, width = acts_all.shape
    cols = w_all.shape[3]
    experts, rows, _ = master.shape
    _, chunks, _, crows, _ = grad_send.shape
    owners = nep // sides
    partner = dp + 1 - 2 * lax.rem(dp, 2)
    near = ep // owners
    quarter = ep // max(nep // 4, 1)
    outer = jnp.where((quarter == 0) | (quarter == 3), 0, 1)
    order = [lax.rem(near + outer + n, sides) for n in range(sides)]
    first = [jnp.where(side == near, 1, 0) for side in order]
    away = [lax.rem(near + 1 + n, sides) for n in range(sides)]
    skip = [0] * (sides - 1) + [1]
    place = lax.rem(ep, owners)

    def target(n_side, k):
        base = n_side * owners
        up = base + owners - 1 - k
        down = base + k
        other = jnp.where(n_side > near, up, down)
        mine = base + lax.rem(place + k, owners)
        return jnp.where(n_side == near, mine, other)

    def local(src, dst, sem):
        return pltpu.make_async_copy(src, dst, sem)

    def remote(src, dst, ssem, rsem, e, d):
        return pltpu.make_async_remote_copy(
            src_ref=src, dst_ref=dst, send_sem=ssem, recv_sem=rsem,
            device_id=(e, d), device_id_type=MESH)

    tables = [local(src, dst, table_sem.at[n]) for n, (src, dst) in
              enumerate(((counts_hbm, counts_ref), (old_hbm, old_ref), (new_hbm, new_ref)))]
    load_grads = local(grads_hbm, g_in, load_sem.at[0])
    load_w = local(w_hbm, w_all.at[dp], load_sem.at[1])
    load_opt = [local(src, dst, load_sem.at[2 + n]) for n, (src, dst) in
                enumerate(((master_hbm, master), (one_hbm, one), (two_hbm, two)))]
    load_acts = [local(acts_hbm.at[:, :, pl.ds(h * width, width)], acts_all.at[h, dp], load_sem.at[5 + h])
                 for h in range(sides)]
    tables[0].start()
    for c in load_acts:
        c.start()
    load_grads.start()
    for c in tables[1:]:
        c.start()
    load_w.start()
    for c in load_opt:
        c.start()

    gate = ndp - 1
    barrier = pltpu.get_barrier_semaphore()
    for k in range(1, ndp):
        to = lax.rem(dp + k, ndp)

        @pl.when(to != gate)
        def _():
            pl.semaphore_signal(barrier, inc=1, device_id=(ep, to), device_id_type=MESH)

    @pl.when(dp != gate)
    def _():
        pl.semaphore_wait(barrier, ndp - 1)

    @pl.when(dp == gate - 1)
    def _():
        pl.semaphore_signal(joined, inc=1, device_id=(ep, gate), device_id_type=MESH)

    @pl.when(dp == gate)
    def _():
        pl.semaphore_wait(joined, 1)

        @pl.loop(1, nep)
        def _(k):
            pl.semaphore_signal(barrier, inc=1, device_id=(lax.rem(ep + k, nep), gate), device_id_type=MESH)

    def open_gate():
        @pl.when(dp == gate)
        def _():
            pl.semaphore_wait(barrier, nep - 1)
            for j in range(gate):
                pl.semaphore_signal(opened, inc=1, device_id=(ep, j), device_id_type=MESH)

    def pass_gate():
        @pl.when(dp != gate)
        def _():
            pl.semaphore_wait(opened, 1)

    def grad_copy(k, s):
        to = lax.rem(dp - k + ndp, ndp)
        return remote(g_send.at[to, s], g_cols.at[dp, s], gs_sem.at[k - 1, s], gr_sem.at[k - 1, s], ep, to)

    def grad_arrival(k, s):
        came = g_cols.at[lax.rem(dp + k, ndp), s]
        return remote(came, came, gs_sem.at[k - 1, s], gr_sem.at[k - 1, s], ep, partner)

    def block_copy(view, k, ssem, rsem):
        own = view(dp)
        to = partner if k == 0 else lax.rem(dp - 2 * k + ndp, ndp)
        return remote(own, own, ssem(k), rsem(k), ep, to)

    def block_arrival(view, k, ssem, rsem):
        if k == 0:
            came = view(partner)
        elif k < half:
            came = view(lax.rem(dp + 2 * k, ndp))
        else:
            came = view(lax.rem(partner + 2 * (k - half + 1), ndp))
        return remote(came, came, ssem(k), rsem(k), ep, partner)

    def block_relay(view, k, ssem, rsem):
        block = view(lax.rem(dp + 2 * k, ndp))
        return remote(block, block, ssem(half - 1 + k), rsem(half - 1 + k), ep, partner)

    def acts_kit(b):
        n, s, low, high = blocks[b]
        return (lambda i: acts_all.at[away[n], i, s, :, pl.ds(low, high - low)],
                lambda k: act_send_sem.at[k, b], lambda k: act_recv_sem.at[k, b])

    def w_kit(s):
        return (lambda i: w_all.at[i, s], lambda k: w_send_sem.at[k, s], lambda k: w_recv_sem.at[k, s])

    def send_block(view, ssem, rsem):
        for k in range(half - 1, -1, -1):
            block_copy(view, k, ssem, rsem).start()

    def relay_block(view, ssem, rsem):
        for k in range(1, half):
            block_arrival(view, k, ssem, rsem).wait_recv()
            block_relay(view, k, ssem, rsem).start()

    def finish_block(view, ssem, rsem):
        block_arrival(view, 0, ssem, rsem).wait_recv()
        for k in range(half, ndp - 1):
            block_arrival(view, k, ssem, rsem).wait_recv()

    pieces = [(n, s) for n in range(sides) for s in range(slots)]
    blocks = piece_blocks(sides, slots, width)

    for c in load_acts:
        c.wait()
    send_block(*acts_kit(0))
    tables[0].wait()
    load_grads.wait()
    for s in range(slots):
        live = (lax.broadcasted_iota(jnp.int32, (toks, 1), 0) < counts_ref[s]).astype(jnp.float32)
        masked = g_in[s] * live
        g_mask[s] = masked
        for j in range(ndp):
            g_send[j, s] = masked[:, j * cols:(j + 1) * cols]
        g_cols[dp, s] = g_send[dp, s]
        for k in range(ndp - 1, 0, -1):
            grad_copy(k, s).start()
        if s == 0:
            for b, (n, t, _, _) in enumerate(blocks):
                if b and (n, t) == pieces[0]:
                    send_block(*acts_kit(b))
    for b, (n, s, _, _) in enumerate(blocks):
        if (n, s) != pieces[0]:
            send_block(*acts_kit(b))
    load_w.wait()
    for s in range(slots):
        send_block(*w_kit(s))

    def send_grad(n, s, c):
        @pl.loop(skip[n], owners)
        def _(k):
            to = target(away[n], k)
            remote(grad_send.at[s, c, to], arrived.at[s, c, ep], es_sem.at[s, c], er_sem.at[s, c], to, dp).start()

    def send_some(n, s, start, stop):
        base = away[n] * owners

        @pl.loop(start, stop)
        def _(i):
            to = base + i

            @pl.when(to != ep)
            def _():
                for c in range(chunks):
                    remote(grad_send.at[s, c, to], arrived.at[s, c, ep], es_sem.at[s, c], er_sem.at[s, c], to, dp).start()

    rights = {}
    for b, (n, s, low, high) in enumerate(blocks):
        relay_block(*acts_kit(b))
        if b == 0:
            open_gate()
        if s not in rights:
            for k in range(1, ndp):
                grad_arrival(k, s).wait_recv()
            rights[s] = split(g_cols[:, s].reshape(ndp * toks, cols))
        finish_block(*acts_kit(b))
        left = split(acts_all[away[n], :, s, :, low:high].reshape(ndp * toks, high - low))
        grad = dot3(left, rights[s], ((0,), (0,)))
        base = away[n] * owners
        for i in range(owners):
            for c in range(chunks):
                at = i * rows + c * crows
                start, stop = max(at, low), min(at + crows, high)
                if start < stop:
                    grad_send[s, c, base + i, start - at:stop - at] = grad[start - low:stop - low]
        if b == 0:
            pass_gate()
        if (n, s) == pieces[0]:
            send_some(n, s, low // rows, high // rows)
        else:
            send_grad(n, s, 0)
    for c in range(1, chunks):
        for n, s in pieces[1:]:
            send_grad(n, s, c)
    for s in range(slots):
        for c in range(chunks):
            arrived[s, c, ep] = grad_send[s, c, ep]

    for c in tables[1:] + load_opt:
        c.wait()

    direct = rows % 8 == 0

    def landing(s, c, i):
        if direct:
            return ns_refs[s].at[pl.ds(pl.multiple_of(i * rows + c * crows, 8), crows)]
        return pick_recv.at[s, i]

    own_stores = []
    for c in range(chunks):
        for s in range(slots):
            came = arrived.at[s, c, pl.ds(0, nep - 1)]
            remote(came, came, es_sem.at[s, c], er_sem.at[s, c], ep, partner).wait_recv()
        span = slice(c * crows, (c + 1) * crows)

        @pl.loop(0, experts)
        def _(e):
            total = jnp.zeros((crows, cols), jnp.float32)
            for i in range(nep):
                for s in range(slots):
                    held = jnp.where(old_ref[i * slots + s] == e, 1.0, 0.0)
                    total = total + held * arrived[s, c, i]
            master[e, span], one[e, span], two[e, span] = adamw(
                master[e, span], one[e, span], two[e, span], total)

        def send_pick(to):
            for s in range(slots):
                pick_send[s, c, to] = master[new_ref[to * slots + s], span]
            for s in range(slots):
                remote(pick_send.at[s, c, to], landing(s, c, ep), ps_sem.at[s, c], pr_sem.at[s, c], to, dp).start()

        for n in range(sides):
            @pl.loop(first[n], owners)
            def _(k):
                send_pick(target(order[n], k))

        for s in range(slots):
            pick_send[s, c, ep] = master[new_ref[ep * slots + s], span]
            own_stores.append(local(pick_send.at[s, c, ep], landing(s, c, ep), store_sem.at[5 + s, c]))
            own_stores[-1].start()

    stores = [local(src, dst, store_sem.at[n, 0]) for n, (src, dst) in
              enumerate(((master, nm_ref), (one, no_ref), (two, nt_ref)))]
    for c in stores:
        c.start()

    for s in range(slots):
        relay_block(*w_kit(s))
    last = []
    for s in range(slots):
        finish_block(*w_kit(s))
        live = (lax.broadcasted_iota(jnp.int32, (toks, 1), 0) < counts_ref[s]).astype(jnp.float32)
        acts = [split(acts_all[h, dp, s] * live) for h in range(sides)]
        back = [jnp.zeros((toks, width), jnp.float32) for h in range(sides)]
        for j in range(ndp):
            at = slice(j * cols, (j + 1) * cols)
            grads = split(g_mask[s, :, at])
            total = jnp.zeros((toks, cols), jnp.float32)
            for h in range(sides):
                weights = split(w_all[j, s, h * width:(h + 1) * width])
                total = total + dot3(acts[h], weights, ((1,), (0,)))
                back[h] = back[h] + dot3(grads, weights, ((1,), (1,)))
            out_v[s, :, at] = total
        for h in range(sides):
            ig_v[s, :, h * width:(h + 1) * width] = back[h]
    last = [local(out_v, out_ref, store_sem.at[3, 0]), local(ig_v, ig_ref, store_sem.at[4, 0])]
    for c in last:
        c.start()

    for s in range(slots):
        for k in range(1, ndp):
            grad_copy(k, s).wait_send()
    for kit in [acts_kit(b) for b in range(len(blocks))] + [w_kit(s) for s in range(slots)]:
        for k in range(half):
            block_copy(kit[0], k, *kit[1:]).wait_send()
        for k in range(1, half):
            block_relay(kit[0], k, *kit[1:]).wait_send()
    for s in range(slots):
        for c in range(chunks):
            gone = grad_send.at[s, c, pl.ds(0, nep - 1)]
            remote(gone, gone, es_sem.at[s, c], er_sem.at[s, c], ep, partner).wait_send()
            gone = pick_send.at[s, c, pl.ds(0, nep - 1)]
            remote(gone, gone, ps_sem.at[s, c], pr_sem.at[s, c], ep, partner).wait_send()
    for c in own_stores + stores + last:
        c.wait()
    for s in range(slots):
        for c in range(chunks):
            if direct:
                came = ns_refs[s].at[pl.ds(0, (nep - 1) * crows)]
            else:
                came = pick_recv.at[s, pl.ds(0, nep - 1)]
            remote(came, came, ps_sem.at[s, c], pr_sem.at[s, c], ep, partner).wait_recv()
    if not direct:
        for s in range(slots):
            for i in range(nep):
                w_all[0, s, i * rows:(i + 1) * rows] = pick_recv[s, i]
            done = local(w_all.at[0, s], ns_refs[s], store_sem.at[0, 0])
            done.start()
            done.wait()


def write_out(slots, *refs):
    ins, outs, sems = refs[:5 + slots], refs[5 + slots:-1], refs[-1]
    parts = list(outs[:5]) + [outs[5].at[n] for n in range(slots)]
    copies = [pltpu.make_async_copy(src, dst, sems.at[n]) for n, (src, dst) in enumerate(zip(ins, parts))]
    for c in copies:
        c.start()
    for c in copies:
        c.wait()


def local_step(nep, ndp, activations, out_grads, counts, slot_weights, master, moment_one, moment_two, old_table, new_table):
    f32 = jnp.float32
    slots, toks, ff = activations.shape
    ds = out_grads.shape[2]
    cols = slot_weights.shape[2]
    experts, rows, _ = master.shape
    direct = rows % 8 == 0
    sides = 2
    chunks = 2 if rows % 16 == 0 else 1
    blocks = len(piece_blocks(sides, slots, ff // sides))
    parted = (slots, chunks, nep, rows // chunks, cols)
    hbm = pl.BlockSpec(memory_space=pl.ANY)
    dma = pltpu.SemaphoreType.DMA
    shapes = [
        jax.ShapeDtypeStruct(x.shape, f32)
        for x in (out_grads, activations, master, moment_one, moment_two, slot_weights)
    ]
    results = pl.pallas_call(
        functools.partial(kernel, nep, ndp, slots),
        out_shape=shapes[:5] + [jax.ShapeDtypeStruct((ff, cols), f32)] * slots,
        in_specs=[hbm] * 9,
        out_specs=[hbm] * (5 + slots),
        scratch_shapes=[
            pltpu.VMEM((sides, ndp, slots, toks, ff // sides), f32),
            pltpu.VMEM((slots, toks, ds), f32),
            pltpu.VMEM((slots, toks, ds), f32),
            pltpu.VMEM((ndp, slots, toks, cols), f32),
            pltpu.VMEM((ndp, slots, toks, cols), f32),
            pltpu.VMEM((ndp, slots, ff, cols), f32),
            pltpu.VMEM(parted, f32),
            pltpu.VMEM(parted, f32),
            pltpu.VMEM((experts, rows, cols), f32),
            pltpu.VMEM((experts, rows, cols), f32),
            pltpu.VMEM((experts, rows, cols), f32),
            pltpu.VMEM(parted, f32),
            pltpu.VMEM((1, 1, 8, 128) if direct else (slots, nep, rows, cols), f32),
            pltpu.VMEM((slots, toks, ds), f32),
            pltpu.VMEM((slots, toks, ff), f32),
            pltpu.SMEM((nep * slots,), jnp.int32),
            pltpu.SMEM((nep * slots,), jnp.int32),
            pltpu.SMEM((slots,), jnp.int32),
            dma((3,)),
            pltpu.SemaphoreType.REGULAR,
            pltpu.SemaphoreType.REGULAR,
            dma((5 + sides,)),
            dma((5 + slots, chunks)),
            dma((ndp - 1, blocks)),
            dma((ndp - 1, blocks)),
            dma((ndp - 1, slots)),
            dma((ndp - 1, slots)),
            dma((ndp - 1, slots)),
            dma((ndp - 1, slots)),
            dma((slots, chunks)),
            dma((slots, chunks)),
            dma((slots, chunks)),
            dma((slots, chunks)),
        ],
        compiler_params=pltpu.CompilerParams(
            collective_id=0, has_side_effects=True, vmem_limit_bytes=VMEM_KIB * 1024
        ),
        name="step",
    )(*[pltpu.with_memory_space_constraint(x, pltpu.HBM) for x in (
        old_table.reshape(-1), new_table.reshape(-1), counts.reshape(-1),
        activations, out_grads, slot_weights, master, moment_one, moment_two)])
    return pl.pallas_call(
        functools.partial(write_out, slots),
        out_shape=shapes,
        in_specs=[hbm] * (5 + slots),
        out_specs=[hbm] * 6,
        scratch_shapes=[dma((5 + slots,))],
        compiler_params=pltpu.CompilerParams(vmem_limit_bytes=1024 * 1024),
        name="write_out",
    )(*results)


def solution(mesh):
    in_specs = (
        P("ep", "dp", None),
        P("ep", "dp", None),
        P("ep", "dp"),
        P("ep", None, "dp"),
        P(None, "ep", "dp"),
        P(None, "ep", "dp"),
        P(None, "ep", "dp"),
        P(),
        P(),
    )
    out_specs = (
        P("ep", "dp", None),
        P("ep", "dp", None),
        P(None, "ep", "dp"),
        P(None, "ep", "dp"),
        P(None, "ep", "dp"),
        P("ep", None, "dp"),
    )
    step = functools.partial(local_step, mesh.shape["ep"], mesh.shape["dp"])
    return jax.shard_map(step, mesh=mesh, in_specs=in_specs, out_specs=out_specs, check_vma=False)
```

```python
import functools
import math

import jax
import jax.numpy as jnp
from jax import lax
from jax.experimental import pallas as pl
from jax.experimental.pallas import tpu as pltpu
from jax.sharding import PartitionSpec as P

STEP = 100
beta_one = 0.9
beta_two = 0.999
learn_rate = 0.02
epsilon = 1e-08
decay_rate = 0.1

MESH = pl.DeviceIdType.MESH


def adamw(master, moment_one, moment_two, expert_grad):
    first_new = beta_one * moment_one + (1.0 - beta_one) * expert_grad
    second_new = beta_two * moment_two + (1.0 - beta_two) * expert_grad * expert_grad
    first_hat = first_new / (1.0 - beta_one**STEP)
    second_hat = second_new / (1.0 - beta_two**STEP)
    updated = master - learn_rate * (
        first_hat / (jnp.sqrt(second_hat) + epsilon) + decay_rate * master
    )
    return (updated, first_new, second_new)


def split(x):
    high = x.astype(jnp.bfloat16)
    low = (x - high.astype(jnp.float32)).astype(jnp.bfloat16)
    return high, low


def dot3(a, b, dims):
    def one(p, q):
        return lax.dot_general(p, q, (dims, ((), ())), preferred_element_type=jnp.float32)

    return one(a[0], b[0]) + (one(a[0], b[1]) + one(a[1], b[0]))


VMEM_KIB = 52400


def piece_blocks(sides, slots, width):
    step = 128 if width % 128 == 0 else width
    found = []
    for s in range(slots):
        for n in range(sides):
            size = step if n == 0 and s == 0 else width
            found += [(n, s, low, low + size) for low in range(0, width, size)]
    return found


def kernel(nep, ndp, slots, *refs):
    old_hbm, new_hbm, counts_hbm, acts_hbm, grads_hbm, w_hbm, master_hbm, one_hbm, two_hbm = refs[:9]
    out_ref, ig_ref, nm_ref, no_ref, nt_ref = refs[9:14]
    ns_refs = refs[14:14 + slots]
    (
        acts_all, g_in, g_mask, g_send, g_cols, w_all, grad_send, arrived,
        master, one, two, pick_send, pick_recv, out_v, ig_v,
        old_ref, new_ref, counts_ref, table_sem, joined, opened,
        load_sem, store_sem,
        act_send_sem, act_recv_sem, w_send_sem, w_recv_sem, gs_sem, gr_sem,
        es_sem, er_sem, ps_sem, pr_sem,
    ) = refs[14 + slots:]
    ep = lax.axis_index("ep")
    dp = lax.axis_index("dp")
    half = ndp // 2
    sides, _, _, toks, width = acts_all.shape
    cols = w_all.shape[3]
    experts, rows, _ = master.shape
    _, chunks, _, crows, _ = grad_send.shape
    owners = nep // sides
    partner = dp + 1 - 2 * lax.rem(dp, 2)
    near = ep // owners
    quarter = ep // max(nep // 4, 1)
    outer = jnp.where((quarter == 0) | (quarter == 3), 0, 1)
    order = [lax.rem(near + outer + n, sides) for n in range(sides)]
    first = [jnp.where(side == near, 1, 0) for side in order]
    away = [lax.rem(near + 1 + n, sides) for n in range(sides)]
    skip = [0] * (sides - 1) + [1]
    place = lax.rem(ep, owners)

    def target(n_side, k):
        base = n_side * owners
        up = base + owners - 1 - k
        down = base + k
        other = jnp.where(n_side > near, up, down)
        mine = base + lax.rem(place + k, owners)
        return jnp.where(n_side == near, mine, other)

    def local(src, dst, sem):
        return pltpu.make_async_copy(src, dst, sem)

    def remote(src, dst, ssem, rsem, e, d):
        return pltpu.make_async_remote_copy(
            src_ref=src, dst_ref=dst, send_sem=ssem, recv_sem=rsem,
            device_id=(e, d), device_id_type=MESH)

    tables = [local(src, dst, table_sem.at[n]) for n, (src, dst) in
              enumerate(((counts_hbm, counts_ref), (old_hbm, old_ref), (new_hbm, new_ref)))]
    load_grads = [local(grads_hbm.at[s], g_in.at[s], load_sem.at[s]) for s in range(slots)]
    load_w = local(w_hbm, w_all.at[dp], load_sem.at[slots])
    load_opt = [local(src, dst, load_sem.at[slots + 1 + n]) for n, (src, dst) in
                enumerate(((master_hbm, master), (one_hbm, one), (two_hbm, two)))]
    pieces = [(n, s) for s in range(slots) for n in range(sides)]
    blocks = piece_blocks(sides, slots, width)

    def load_block(b):
        n, s, low, high = blocks[b]
        start = pl.multiple_of(away[n] * width + low, math.gcd(width, 128))
        return local(acts_hbm.at[s, :, pl.ds(start, high - low)], acts_all.at[away[n], dp, s, :, pl.ds(low, high - low)],
                     load_sem.at[slots + 4 + b])

    load_block(0).start()
    tables[0].start()
    load_grads[0].start()
    for b in range(1, len(blocks)):
        if blocks[b][:2] == pieces[0]:
            load_block(b).start()
    for c in load_grads[1:]:
        c.start()
    for b in range(1, len(blocks)):
        if blocks[b][:2] != pieces[0]:
            load_block(b).start()

    gate = ndp - 1
    barrier = pltpu.get_barrier_semaphore()
    for k in range(1, ndp):
        to = lax.rem(dp + k, ndp)

        @pl.when(to != gate)
        def _():
            pl.semaphore_signal(barrier, inc=1, device_id=(ep, to), device_id_type=MESH)

    @pl.when(dp != gate)
    def _():
        pl.semaphore_wait(barrier, ndp - 1)

    @pl.when(dp == gate - 1)
    def _():
        pl.semaphore_signal(joined, inc=1, device_id=(ep, gate), device_id_type=MESH)

    @pl.when(dp == gate)
    def _():
        pl.semaphore_wait(joined, 1)

        @pl.loop(1, nep)
        def _(k):
            pl.semaphore_signal(barrier, inc=1, device_id=(lax.rem(ep + k, nep), gate), device_id_type=MESH)

    def open_gate():
        @pl.when(dp == gate)
        def _():
            pl.semaphore_wait(barrier, nep - 1)
            for j in range(gate):
                pl.semaphore_signal(opened, inc=1, device_id=(ep, j), device_id_type=MESH)

    def pass_gate():
        @pl.when(dp != gate)
        def _():
            pl.semaphore_wait(opened, 1)

    def grad_copy(k, s):
        to = lax.rem(dp - k + ndp, ndp)
        return remote(g_send.at[to, s], g_cols.at[dp, s], gs_sem.at[k - 1, s], gr_sem.at[k - 1, s], ep, to)

    def grad_arrival(k, s):
        came = g_cols.at[lax.rem(dp + k, ndp), s]
        return remote(came, came, gs_sem.at[k - 1, s], gr_sem.at[k - 1, s], ep, partner)

    def block_copy(view, k, ssem, rsem):
        own = view(dp)
        to = partner if k == 0 else lax.rem(dp - 2 * k + ndp, ndp)
        return remote(own, own, ssem(k), rsem(k), ep, to)

    def block_arrival(view, k, ssem, rsem):
        if k == 0:
            came = view(partner)
        elif k < half:
            came = view(lax.rem(dp + 2 * k, ndp))
        else:
            came = view(lax.rem(partner + 2 * (k - half + 1), ndp))
        return remote(came, came, ssem(k), rsem(k), ep, partner)

    def block_relay(view, k, ssem, rsem):
        block = view(lax.rem(dp + 2 * k, ndp))
        return remote(block, block, ssem(half - 1 + k), rsem(half - 1 + k), ep, partner)

    def acts_kit(b):
        n, s, low, high = blocks[b]
        return (lambda i: acts_all.at[away[n], i, s, :, pl.ds(low, high - low)],
                lambda k: act_send_sem.at[k, b], lambda k: act_recv_sem.at[k, b])

    def w_kit(s):
        return (lambda i: w_all.at[i, s], lambda k: w_send_sem.at[k, s], lambda k: w_recv_sem.at[k, s])

    def send_block(view, ssem, rsem):
        for k in range(half - 1, -1, -1):
            block_copy(view, k, ssem, rsem).start()

    def relay_block(view, ssem, rsem):
        for k in range(1, half):
            block_arrival(view, k, ssem, rsem).wait_recv()
            block_relay(view, k, ssem, rsem).start()

    def finish_block(view, ssem, rsem):
        block_arrival(view, 0, ssem, rsem).wait_recv()
        for k in range(half, ndp - 1):
            block_arrival(view, k, ssem, rsem).wait_recv()

    load_block(0).wait()
    send_block(*acts_kit(0))
    tables[0].wait()
    for s in range(slots):
        load_grads[s].wait()
        live = (lax.broadcasted_iota(jnp.int32, (toks, 1), 0) < counts_ref[s]).astype(jnp.float32)
        masked = g_in[s] * live
        for j in range(ndp):
            g_send[j, s] = masked[:, j * cols:(j + 1) * cols]
        for k in range(ndp - 1, 0, -1):
            grad_copy(k, s).start()
        if s == 0:
            for b in range(1, len(blocks)):
                if blocks[b][:2] == pieces[0]:
                    load_block(b).wait()
                    send_block(*acts_kit(b))
            load_w.start()
            for c in tables[1:] + load_opt:
                c.start()
        g_mask[s] = masked
        g_cols[dp, s] = g_send[dp, s]
    for b in range(1, len(blocks)):
        if blocks[b][:2] != pieces[0]:
            load_block(b).wait()
            send_block(*acts_kit(b))
    load_w.wait()
    for s in range(slots):
        send_block(*w_kit(s))

    def send_grad(n, s, c):
        @pl.loop(skip[n], owners)
        def _(k):
            to = target(away[n], k)
            remote(grad_send.at[s, c, to], arrived.at[s, c, ep], es_sem.at[s, c], er_sem.at[s, c], to, dp).start()

    def send_some(n, s, start, stop):
        base = away[n] * owners

        @pl.loop(start, stop)
        def _(i):
            to = base + i

            @pl.when(to != ep)
            def _():
                for c in range(chunks):
                    remote(grad_send.at[s, c, to], arrived.at[s, c, ep], es_sem.at[s, c], er_sem.at[s, c], to, dp).start()

    rights = {}
    for b, (n, s, low, high) in enumerate(blocks):
        relay_block(*acts_kit(b))
        if b == 0:
            open_gate()
        finish_block(*acts_kit(b))
        left = split(acts_all[away[n], :, s, :, low:high].reshape(ndp * toks, high - low))
        if s not in rights:
            for k in range(1, ndp):
                grad_arrival(k, s).wait_recv()
            rights[s] = split(g_cols[:, s].reshape(ndp * toks, cols))
        grad = dot3(left, rights[s], ((0,), (0,)))
        base = away[n] * owners
        for i in range(owners):
            for c in range(chunks):
                at = i * rows + c * crows
                start, stop = max(at, low), min(at + crows, high)
                if start < stop:
                    grad_send[s, c, base + i, start - at:stop - at] = grad[start - low:stop - low]
        if b == 0:
            pass_gate()
        if (n, s) == pieces[0]:
            send_some(n, s, low // rows, high // rows)
        else:
            send_grad(n, s, 0)
    for c in range(1, chunks):
        for n, s in pieces[1:]:
            send_grad(n, s, c)
    for s in range(slots):
        for c in range(chunks):
            arrived[s, c, ep] = grad_send[s, c, ep]

    for c in tables[1:] + load_opt:
        c.wait()

    direct = rows % 8 == 0

    def landing(s, c, i):
        if direct:
            return ns_refs[s].at[pl.ds(pl.multiple_of(i * rows + c * crows, 8), crows)]
        return pick_recv.at[s, i]

    own_stores = []
    for c in range(chunks):
        for s in range(slots):
            came = arrived.at[s, c, pl.ds(0, nep - 1)]
            remote(came, came, es_sem.at[s, c], er_sem.at[s, c], ep, partner).wait_recv()
        span = slice(c * crows, (c + 1) * crows)

        @pl.loop(0, experts)
        def _(e):
            total = jnp.zeros((crows, cols), jnp.float32)
            for i in range(nep):
                for s in range(slots):
                    held = jnp.where(old_ref[i * slots + s] == e, 1.0, 0.0)
                    total = total + held * arrived[s, c, i]
            master[e, span], one[e, span], two[e, span] = adamw(
                master[e, span], one[e, span], two[e, span], total)

        def send_pick(to):
            for s in range(slots):
                pick_send[s, c, to] = master[new_ref[to * slots + s], span]
            for s in range(slots):
                remote(pick_send.at[s, c, to], landing(s, c, ep), ps_sem.at[s, c], pr_sem.at[s, c], to, dp).start()

        for n in range(sides):
            @pl.loop(first[n], owners)
            def _(k):
                send_pick(target(order[n], k))

        for s in range(slots):
            pick_send[s, c, ep] = master[new_ref[ep * slots + s], span]
            own_stores.append(local(pick_send.at[s, c, ep], landing(s, c, ep), store_sem.at[5 + s, c]))
            own_stores[-1].start()

    stores = [local(src, dst, store_sem.at[n, 0]) for n, (src, dst) in
              enumerate(((master, nm_ref), (one, no_ref), (two, nt_ref)))]
    for c in stores:
        c.start()

    for s in range(slots):
        relay_block(*w_kit(s))
    last = []
    for s in range(slots):
        finish_block(*w_kit(s))
        live = (lax.broadcasted_iota(jnp.int32, (toks, 1), 0) < counts_ref[s]).astype(jnp.float32)
        acts = [split(acts_all[h, dp, s] * live) for h in range(sides)]
        back = [jnp.zeros((toks, width), jnp.float32) for h in range(sides)]
        for j in range(ndp):
            at = slice(j * cols, (j + 1) * cols)
            grads = split(g_mask[s, :, at])
            total = jnp.zeros((toks, cols), jnp.float32)
            for h in range(sides):
                weights = split(w_all[j, s, h * width:(h + 1) * width])
                total = total + dot3(acts[h], weights, ((1,), (0,)))
                back[h] = back[h] + dot3(grads, weights, ((1,), (1,)))
            out_v[s, :, at] = total
        for h in range(sides):
            ig_v[s, :, h * width:(h + 1) * width] = back[h]
    last = [local(out_v, out_ref, store_sem.at[3, 0]), local(ig_v, ig_ref, store_sem.at[4, 0])]
    for c in last:
        c.start()

    for s in range(slots):
        for k in range(1, ndp):
            grad_copy(k, s).wait_send()
    for kit in [acts_kit(b) for b in range(len(blocks))] + [w_kit(s) for s in range(slots)]:
        for k in range(half):
            block_copy(kit[0], k, *kit[1:]).wait_send()
        for k in range(1, half):
            block_relay(kit[0], k, *kit[1:]).wait_send()
    for s in range(slots):
        for c in range(chunks):
            gone = grad_send.at[s, c, pl.ds(0, nep - 1)]
            remote(gone, gone, es_sem.at[s, c], er_sem.at[s, c], ep, partner).wait_send()
            gone = pick_send.at[s, c, pl.ds(0, nep - 1)]
            remote(gone, gone, ps_sem.at[s, c], pr_sem.at[s, c], ep, partner).wait_send()
    for c in own_stores + stores + last:
        c.wait()
    for s in range(slots):
        for c in range(chunks):
            if direct:
                came = ns_refs[s].at[pl.ds(0, (nep - 1) * crows)]
            else:
                came = pick_recv.at[s, pl.ds(0, nep - 1)]
            remote(came, came, ps_sem.at[s, c], pr_sem.at[s, c], ep, partner).wait_recv()
    if not direct:
        for s in range(slots):
            for i in range(nep):
                w_all[0, s, i * rows:(i + 1) * rows] = pick_recv[s, i]
            done = local(w_all.at[0, s], ns_refs[s], store_sem.at[0, 0])
            done.start()
            done.wait()


def write_out(slots, *refs):
    ins, outs, sems = refs[:5 + slots], refs[5 + slots:-1], refs[-1]
    parts = list(outs[:5]) + [outs[5].at[n] for n in range(slots)]
    copies = [pltpu.make_async_copy(src, dst, sems.at[n]) for n, (src, dst) in enumerate(zip(ins, parts))]
    for c in copies:
        c.start()
    for c in copies:
        c.wait()


def local_step(nep, ndp, activations, out_grads, counts, slot_weights, master, moment_one, moment_two, old_table, new_table):
    f32 = jnp.float32
    slots, toks, ff = activations.shape
    ds = out_grads.shape[2]
    cols = slot_weights.shape[2]
    experts, rows, _ = master.shape
    direct = rows % 8 == 0
    sides = 2
    chunks = 2 if rows % 16 == 0 else 1
    blocks = len(piece_blocks(sides, slots, ff // sides))
    parted = (slots, chunks, nep, rows // chunks, cols)
    hbm = pl.BlockSpec(memory_space=pl.ANY)
    dma = pltpu.SemaphoreType.DMA
    shapes = [
        jax.ShapeDtypeStruct(x.shape, f32)
        for x in (out_grads, activations, master, moment_one, moment_two, slot_weights)
    ]
    results = pl.pallas_call(
        functools.partial(kernel, nep, ndp, slots),
        out_shape=shapes[:5] + [jax.ShapeDtypeStruct((ff, cols), f32)] * slots,
        in_specs=[hbm] * 9,
        out_specs=[hbm] * (5 + slots),
        scratch_shapes=[
            pltpu.VMEM((sides, ndp, slots, toks, ff // sides), f32),
            pltpu.VMEM((slots, toks, ds), f32),
            pltpu.VMEM((slots, toks, ds), f32),
            pltpu.VMEM((ndp, slots, toks, cols), f32),
            pltpu.VMEM((ndp, slots, toks, cols), f32),
            pltpu.VMEM((ndp, slots, ff, cols), f32),
            pltpu.VMEM(parted, f32),
            pltpu.VMEM(parted, f32),
            pltpu.VMEM((experts, rows, cols), f32),
            pltpu.VMEM((experts, rows, cols), f32),
            pltpu.VMEM((experts, rows, cols), f32),
            pltpu.VMEM(parted, f32),
            pltpu.VMEM((1, 1, 8, 128) if direct else (slots, nep, rows, cols), f32),
            pltpu.VMEM((slots, toks, ds), f32),
            pltpu.VMEM((slots, toks, ff), f32),
            pltpu.SMEM((nep * slots,), jnp.int32),
            pltpu.SMEM((nep * slots,), jnp.int32),
            pltpu.SMEM((slots,), jnp.int32),
            dma((3,)),
            pltpu.SemaphoreType.REGULAR,
            pltpu.SemaphoreType.REGULAR,
            dma((slots + 4 + blocks,)),
            dma((5 + slots, chunks)),
            dma((ndp - 1, blocks)),
            dma((ndp - 1, blocks)),
            dma((ndp - 1, slots)),
            dma((ndp - 1, slots)),
            dma((ndp - 1, slots)),
            dma((ndp - 1, slots)),
            dma((slots, chunks)),
            dma((slots, chunks)),
            dma((slots, chunks)),
            dma((slots, chunks)),
        ],
        compiler_params=pltpu.CompilerParams(
            collective_id=0, has_side_effects=True, vmem_limit_bytes=VMEM_KIB * 1024
        ),
        name="step",
    )(*[pltpu.with_memory_space_constraint(x, pltpu.HBM) for x in (
        old_table.reshape(-1), new_table.reshape(-1), counts.reshape(-1),
        activations, out_grads, slot_weights, master, moment_one, moment_two)])
    return pl.pallas_call(
        functools.partial(write_out, slots),
        out_shape=shapes,
        in_specs=[hbm] * (5 + slots),
        out_specs=[hbm] * 6,
        scratch_shapes=[dma((5 + slots,))],
        compiler_params=pltpu.CompilerParams(vmem_limit_bytes=1024 * 1024),
        name="write_out",
    )(*results)


def solution(mesh):
    in_specs = (
        P("ep", "dp", None),
        P("ep", "dp", None),
        P("ep", "dp"),
        P("ep", None, "dp"),
        P(None, "ep", "dp"),
        P(None, "ep", "dp"),
        P(None, "ep", "dp"),
        P(),
        P(),
    )
    out_specs = (
        P("ep", "dp", None),
        P("ep", "dp", None),
        P(None, "ep", "dp"),
        P(None, "ep", "dp"),
        P(None, "ep", "dp"),
        P("ep", None, "dp"),
    )
    step = functools.partial(local_step, mesh.shape["ep"], mesh.shape["dp"])
    return jax.shard_map(step, mesh=mesh, in_specs=in_specs, out_specs=out_specs, check_vma=False)
```

```python
import functools
import math

import jax
import jax.numpy as jnp
from jax import lax
from jax.experimental import pallas as pl
from jax.experimental.pallas import tpu as pltpu
from jax.sharding import PartitionSpec as P

STEP = 100
beta_one = 0.9
beta_two = 0.999
learn_rate = 0.02
epsilon = 1e-08
decay_rate = 0.1

MESH = pl.DeviceIdType.MESH


def adamw(master, moment_one, moment_two, expert_grad):
    first_new = beta_one * moment_one + (1.0 - beta_one) * expert_grad
    second_new = beta_two * moment_two + (1.0 - beta_two) * expert_grad * expert_grad
    first_hat = first_new / (1.0 - beta_one**STEP)
    second_hat = second_new / (1.0 - beta_two**STEP)
    updated = master - learn_rate * (
        first_hat / (jnp.sqrt(second_hat) + epsilon) + decay_rate * master
    )
    return (updated, first_new, second_new)


def split(x):
    high = x.astype(jnp.bfloat16)
    low = (x - high.astype(jnp.float32)).astype(jnp.bfloat16)
    return high, low


def dot3(a, b, dims):
    def one(p, q):
        return lax.dot_general(p, q, (dims, ((), ())), preferred_element_type=jnp.float32)

    return one(a[0], b[0]) + (one(a[0], b[1]) + one(a[1], b[0]))


VMEM_KIB = 52400


def piece_blocks(sides, slots, width):
    step = 128 if width % 128 == 0 else width
    found = []
    for s in range(slots):
        for n in range(sides):
            size = step if n == 0 and s == 0 else width
            found += [(n, s, low, low + size) for low in range(0, width, size)]
    return found


def kernel(nep, ndp, slots, *refs):
    old_hbm, new_hbm, counts_hbm, acts_hbm, grads_hbm, w_hbm, master_hbm, one_hbm, two_hbm = refs[:9]
    out_ref, ig_ref, nm_ref, no_ref, nt_ref = refs[9:14]
    ns_refs = refs[14:14 + slots]
    (
        acts_all, g_in, g_mask, g_send, g_cols, w_all, grad_send, arrived,
        master, one, two, pick_send, pick_recv, out_v, ig_v,
        old_ref, new_ref, counts_ref, table_sem, joined, opened,
        load_sem, store_sem,
        act_send_sem, act_recv_sem, w_send_sem, w_recv_sem, gs_sem, gr_sem,
        es_sem, er_sem, ps_sem, pr_sem,
    ) = refs[14 + slots:]
    ep = lax.axis_index("ep")
    dp = lax.axis_index("dp")
    half = ndp // 2
    sides, _, _, toks, width = acts_all.shape
    cols = w_all.shape[3]
    experts, rows, _ = master.shape
    _, chunks, _, crows, _ = grad_send.shape
    owners = nep // sides
    partner = dp + 1 - 2 * lax.rem(dp, 2)
    near = ep // owners
    quarter = ep // max(nep // 4, 1)
    outer = jnp.where((quarter == 0) | (quarter == 3), 0, 1)
    order = [lax.rem(near + outer + n, sides) for n in range(sides)]
    first = [jnp.where(side == near, 1, 0) for side in order]
    away = [lax.rem(near + 1 + n, sides) for n in range(sides)]
    skip = [0] * (sides - 1) + [1]
    place = lax.rem(ep, owners)

    def target(n_side, k):
        base = n_side * owners
        up = base + owners - 1 - k
        down = base + k
        other = jnp.where(n_side > near, up, down)
        mine = base + lax.rem(place + k, owners)
        return jnp.where(n_side == near, mine, other)

    def local(src, dst, sem):
        return pltpu.make_async_copy(src, dst, sem)

    def remote(src, dst, ssem, rsem, e, d):
        return pltpu.make_async_remote_copy(
            src_ref=src, dst_ref=dst, send_sem=ssem, recv_sem=rsem,
            device_id=(e, d), device_id_type=MESH)

    tables = [local(src, dst, table_sem.at[n]) for n, (src, dst) in
              enumerate(((counts_hbm, counts_ref), (old_hbm, old_ref), (new_hbm, new_ref)))]
    load_grads = [local(grads_hbm.at[s], g_in.at[s], load_sem.at[s]) for s in range(slots)]
    load_w = local(w_hbm, w_all.at[dp], load_sem.at[slots])
    load_opt = [local(src, dst, load_sem.at[slots + 1 + n]) for n, (src, dst) in
                enumerate(((master_hbm, master), (one_hbm, one), (two_hbm, two)))]
    pieces = [(n, s) for s in range(slots) for n in range(sides)]
    blocks = piece_blocks(sides, slots, width)

    def load_block(b):
        n, s, low, high = blocks[b]
        start = pl.multiple_of(away[n] * width + low, math.gcd(width, 128))
        return local(acts_hbm.at[s, :, pl.ds(start, high - low)], acts_all.at[away[n], dp, s, :, pl.ds(low, high - low)],
                     load_sem.at[slots + 4 + b])

    load_block(0).start()
    tables[0].start()
    load_grads[0].start()
    for b in range(1, len(blocks)):
        if blocks[b][:2] == pieces[0]:
            load_block(b).start()
    for c in load_grads[1:]:
        c.start()
    for b in range(1, len(blocks)):
        if blocks[b][:2] != pieces[0]:
            load_block(b).start()

    gate = ndp - 1
    barrier = pltpu.get_barrier_semaphore()
    for k in range(1, ndp):
        to = lax.rem(dp + k, ndp)

        @pl.when(to != gate)
        def _():
            pl.semaphore_signal(barrier, inc=1, device_id=(ep, to), device_id_type=MESH)

    @pl.when(dp != gate)
    def _():
        pl.semaphore_wait(barrier, ndp - 1)

    @pl.when(dp == gate - 1)
    def _():
        pl.semaphore_signal(joined, inc=1, device_id=(ep, gate), device_id_type=MESH)

    @pl.when(dp == gate)
    def _():
        pl.semaphore_wait(joined, 1)

        @pl.loop(1, nep)
        def _(k):
            pl.semaphore_signal(barrier, inc=1, device_id=(lax.rem(ep + k, nep), gate), device_id_type=MESH)

    def open_gate():
        @pl.when(dp == gate)
        def _():
            pl.semaphore_wait(barrier, nep - 1)
            for j in range(gate):
                pl.semaphore_signal(opened, inc=1, device_id=(ep, j), device_id_type=MESH)

    def pass_gate():
        @pl.when(dp != gate)
        def _():
            pl.semaphore_wait(opened, 1)

    def grad_copy(k, s):
        to = lax.rem(dp - k + ndp, ndp)
        return remote(g_send.at[to, s], g_cols.at[dp, s], gs_sem.at[k - 1, s], gr_sem.at[k - 1, s], ep, to)

    def grad_arrival(k, s):
        came = g_cols.at[lax.rem(dp + k, ndp), s]
        return remote(came, came, gs_sem.at[k - 1, s], gr_sem.at[k - 1, s], ep, partner)

    def block_copy(view, k, ssem, rsem):
        own = view(dp)
        to = partner if k == 0 else lax.rem(dp - 2 * k + ndp, ndp)
        return remote(own, own, ssem(k), rsem(k), ep, to)

    def block_arrival(view, k, ssem, rsem):
        if k == 0:
            came = view(partner)
        elif k < half:
            came = view(lax.rem(dp + 2 * k, ndp))
        else:
            came = view(lax.rem(partner + 2 * (k - half + 1), ndp))
        return remote(came, came, ssem(k), rsem(k), ep, partner)

    def block_relay(view, k, ssem, rsem):
        block = view(lax.rem(dp + 2 * k, ndp))
        return remote(block, block, ssem(half - 1 + k), rsem(half - 1 + k), ep, partner)

    def acts_kit(b):
        n, s, low, high = blocks[b]
        return (lambda i: acts_all.at[away[n], i, s, :, pl.ds(low, high - low)],
                lambda k: act_send_sem.at[k, b], lambda k: act_recv_sem.at[k, b])

    def w_kit(s):
        return (lambda i: w_all.at[i, s], lambda k: w_send_sem.at[k, s], lambda k: w_recv_sem.at[k, s])

    def send_block(view, ssem, rsem):
        for k in range(half - 1, -1, -1):
            block_copy(view, k, ssem, rsem).start()

    def relay_block(view, ssem, rsem):
        for k in range(1, half):
            block_arrival(view, k, ssem, rsem).wait_recv()
            block_relay(view, k, ssem, rsem).start()

    def finish_block(view, ssem, rsem):
        block_arrival(view, 0, ssem, rsem).wait_recv()
        for k in range(half, ndp - 1):
            block_arrival(view, k, ssem, rsem).wait_recv()

    load_block(0).wait()
    send_block(*acts_kit(0))
    tables[0].wait()
    for s in range(slots):
        load_grads[s].wait()
        live = (lax.broadcasted_iota(jnp.int32, (toks, 1), 0) < counts_ref[s]).astype(jnp.float32)
        masked = g_in[s] * live
        for j in range(ndp):
            g_send[j, s] = masked[:, j * cols:(j + 1) * cols]
        for k in range(ndp - 1, 0, -1):
            grad_copy(k, s).start()
        if s == 0:
            for b in range(1, len(blocks)):
                if blocks[b][:2] == pieces[0]:
                    load_block(b).wait()
                    send_block(*acts_kit(b))
            load_w.start()
            for c in tables[1:] + load_opt:
                c.start()
        g_mask[s] = masked
        g_cols[dp, s] = g_send[dp, s]
    for b in range(1, len(blocks)):
        if blocks[b][:2] != pieces[0]:
            load_block(b).wait()
            send_block(*acts_kit(b))
    load_w.wait()
    for s in range(slots):
        send_block(*w_kit(s))

    def send_grad(n, s, c):
        @pl.loop(skip[n], owners)
        def _(k):
            to = target(away[n], k)
            remote(grad_send.at[s, c, to], arrived.at[s, c, ep], es_sem.at[s, c], er_sem.at[s, c], to, dp).start()

    def send_some(n, s, start, stop):
        base = away[n] * owners

        @pl.loop(start, stop)
        def _(i):
            to = base + i

            @pl.when(to != ep)
            def _():
                for c in range(chunks):
                    remote(grad_send.at[s, c, to], arrived.at[s, c, ep], es_sem.at[s, c], er_sem.at[s, c], to, dp).start()

    seen, turned = set(), {}
    for b, (n, s, low, high) in enumerate(blocks):
        relay_block(*acts_kit(b))
        if b == 0:
            open_gate()
        finish_block(*acts_kit(b))
        left = split(acts_all[away[n], :, s, :, low:high].reshape(ndp * toks, high - low))
        if s not in seen:
            for k in range(1, ndp):
                grad_arrival(k, s).wait_recv()
            seen.add(s)
        if b == 0:
            grad = dot3(left, split(g_cols[:, s].reshape(ndp * toks, cols)), ((0,), (0,)))
        else:
            if s not in turned:
                turned[s] = split(g_cols[:, s].reshape(ndp * toks, cols).T)
            grad = dot3(turned[s], left, ((1,), (0,))).T
        base = away[n] * owners
        for i in range(owners):
            for c in range(chunks):
                at = i * rows + c * crows
                start, stop = max(at, low), min(at + crows, high)
                if start < stop:
                    grad_send[s, c, base + i, start - at:stop - at] = grad[start - low:stop - low]
        if b == 0:
            pass_gate()
        if (n, s) == pieces[0]:
            send_some(n, s, low // rows, high // rows)
        else:
            send_grad(n, s, 0)
    for c in range(1, chunks):
        for n, s in pieces[1:]:
            send_grad(n, s, c)
    for s in range(slots):
        for c in range(chunks):
            arrived[s, c, ep] = grad_send[s, c, ep]

    for c in tables[1:] + load_opt:
        c.wait()

    direct = rows % 8 == 0

    def landing(s, c, i):
        if direct:
            return ns_refs[s].at[pl.ds(pl.multiple_of(i * rows + c * crows, 8), crows)]
        return pick_recv.at[s, i]

    own_stores = []
    for c in range(chunks):
        for s in range(slots):
            came = arrived.at[s, c, pl.ds(0, nep - 1)]
            remote(came, came, es_sem.at[s, c], er_sem.at[s, c], ep, partner).wait_recv()
        span = slice(c * crows, (c + 1) * crows)

        @pl.loop(0, experts)
        def _(e):
            total = jnp.zeros((crows, cols), jnp.float32)
            for i in range(nep):
                for s in range(slots):
                    held = jnp.where(old_ref[i * slots + s] == e, 1.0, 0.0)
                    total = total + held * arrived[s, c, i]
            master[e, span], one[e, span], two[e, span] = adamw(
                master[e, span], one[e, span], two[e, span], total)

        def send_pick(to):
            for s in range(slots):
                pick_send[s, c, to] = master[new_ref[to * slots + s], span]
            for s in range(slots):
                remote(pick_send.at[s, c, to], landing(s, c, ep), ps_sem.at[s, c], pr_sem.at[s, c], to, dp).start()

        for n in range(sides):
            @pl.loop(first[n], owners)
            def _(k):
                send_pick(target(order[n], k))

        for s in range(slots):
            pick_send[s, c, ep] = master[new_ref[ep * slots + s], span]
            own_stores.append(local(pick_send.at[s, c, ep], landing(s, c, ep), store_sem.at[5 + s, c]))
            own_stores[-1].start()

    stores = [local(src, dst, store_sem.at[n, 0]) for n, (src, dst) in
              enumerate(((master, nm_ref), (one, no_ref), (two, nt_ref)))]
    for c in stores:
        c.start()

    for s in range(slots):
        relay_block(*w_kit(s))
    last = []
    for s in range(slots):
        finish_block(*w_kit(s))
        live = (lax.broadcasted_iota(jnp.int32, (toks, 1), 0) < counts_ref[s]).astype(jnp.float32)
        acts = [split(acts_all[h, dp, s] * live) for h in range(sides)]
        back = [jnp.zeros((toks, width), jnp.float32) for h in range(sides)]
        for j in range(ndp):
            at = slice(j * cols, (j + 1) * cols)
            grads = split(g_mask[s, :, at])
            total = jnp.zeros((toks, cols), jnp.float32)
            for h in range(sides):
                weights = split(w_all[j, s, h * width:(h + 1) * width])
                total = total + dot3(acts[h], weights, ((1,), (0,)))
                back[h] = back[h] + dot3(grads, weights, ((1,), (1,)))
            out_v[s, :, at] = total
        for h in range(sides):
            ig_v[s, :, h * width:(h + 1) * width] = back[h]
    last = [local(out_v, out_ref, store_sem.at[3, 0]), local(ig_v, ig_ref, store_sem.at[4, 0])]
    for c in last:
        c.start()

    for s in range(slots):
        for k in range(1, ndp):
            grad_copy(k, s).wait_send()
    for kit in [acts_kit(b) for b in range(len(blocks))] + [w_kit(s) for s in range(slots)]:
        for k in range(half):
            block_copy(kit[0], k, *kit[1:]).wait_send()
        for k in range(1, half):
            block_relay(kit[0], k, *kit[1:]).wait_send()
    for s in range(slots):
        for c in range(chunks):
            gone = grad_send.at[s, c, pl.ds(0, nep - 1)]
            remote(gone, gone, es_sem.at[s, c], er_sem.at[s, c], ep, partner).wait_send()
            gone = pick_send.at[s, c, pl.ds(0, nep - 1)]
            remote(gone, gone, ps_sem.at[s, c], pr_sem.at[s, c], ep, partner).wait_send()
    for c in own_stores + stores + last:
        c.wait()
    for s in range(slots):
        for c in range(chunks):
            if direct:
                came = ns_refs[s].at[pl.ds(0, (nep - 1) * crows)]
            else:
                came = pick_recv.at[s, pl.ds(0, nep - 1)]
            remote(came, came, ps_sem.at[s, c], pr_sem.at[s, c], ep, partner).wait_recv()
    if not direct:
        for s in range(slots):
            for i in range(nep):
                w_all[0, s, i * rows:(i + 1) * rows] = pick_recv[s, i]
            done = local(w_all.at[0, s], ns_refs[s], store_sem.at[0, 0])
            done.start()
            done.wait()


def write_out(slots, *refs):
    ins, outs, sems = refs[:5 + slots], refs[5 + slots:-1], refs[-1]
    parts = list(outs[:5]) + [outs[5].at[n] for n in range(slots)]
    copies = [pltpu.make_async_copy(src, dst, sems.at[n]) for n, (src, dst) in enumerate(zip(ins, parts))]
    for c in copies:
        c.start()
    for c in copies:
        c.wait()


def local_step(nep, ndp, activations, out_grads, counts, slot_weights, master, moment_one, moment_two, old_table, new_table):
    f32 = jnp.float32
    slots, toks, ff = activations.shape
    ds = out_grads.shape[2]
    cols = slot_weights.shape[2]
    experts, rows, _ = master.shape
    direct = rows % 8 == 0
    sides = 2
    chunks = 2 if rows % 16 == 0 else 1
    blocks = len(piece_blocks(sides, slots, ff // sides))
    parted = (slots, chunks, nep, rows // chunks, cols)
    hbm = pl.BlockSpec(memory_space=pl.ANY)
    dma = pltpu.SemaphoreType.DMA
    shapes = [
        jax.ShapeDtypeStruct(x.shape, f32)
        for x in (out_grads, activations, master, moment_one, moment_two, slot_weights)
    ]
    results = pl.pallas_call(
        functools.partial(kernel, nep, ndp, slots),
        out_shape=shapes[:5] + [jax.ShapeDtypeStruct((ff, cols), f32)] * slots,
        in_specs=[hbm] * 9,
        out_specs=[hbm] * (5 + slots),
        scratch_shapes=[
            pltpu.VMEM((sides, ndp, slots, toks, ff // sides), f32),
            pltpu.VMEM((slots, toks, ds), f32),
            pltpu.VMEM((slots, toks, ds), f32),
            pltpu.VMEM((ndp, slots, toks, cols), f32),
            pltpu.VMEM((ndp, slots, toks, cols), f32),
            pltpu.VMEM((ndp, slots, ff, cols), f32),
            pltpu.VMEM(parted, f32),
            pltpu.VMEM(parted, f32),
            pltpu.VMEM((experts, rows, cols), f32),
            pltpu.VMEM((experts, rows, cols), f32),
            pltpu.VMEM((experts, rows, cols), f32),
            pltpu.VMEM(parted, f32),
            pltpu.VMEM((1, 1, 8, 128) if direct else (slots, nep, rows, cols), f32),
            pltpu.VMEM((slots, toks, ds), f32),
            pltpu.VMEM((slots, toks, ff), f32),
            pltpu.SMEM((nep * slots,), jnp.int32),
            pltpu.SMEM((nep * slots,), jnp.int32),
            pltpu.SMEM((slots,), jnp.int32),
            dma((3,)),
            pltpu.SemaphoreType.REGULAR,
            pltpu.SemaphoreType.REGULAR,
            dma((slots + 4 + blocks,)),
            dma((5 + slots, chunks)),
            dma((ndp - 1, blocks)),
            dma((ndp - 1, blocks)),
            dma((ndp - 1, slots)),
            dma((ndp - 1, slots)),
            dma((ndp - 1, slots)),
            dma((ndp - 1, slots)),
            dma((slots, chunks)),
            dma((slots, chunks)),
            dma((slots, chunks)),
            dma((slots, chunks)),
        ],
        compiler_params=pltpu.CompilerParams(
            collective_id=0, has_side_effects=True, vmem_limit_bytes=VMEM_KIB * 1024
        ),
        name="step",
    )(*[pltpu.with_memory_space_constraint(x, pltpu.HBM) for x in (
        old_table.reshape(-1), new_table.reshape(-1), counts.reshape(-1),
        activations, out_grads, slot_weights, master, moment_one, moment_two)])
    return pl.pallas_call(
        functools.partial(write_out, slots),
        out_shape=shapes,
        in_specs=[hbm] * (5 + slots),
        out_specs=[hbm] * 6,
        scratch_shapes=[dma((5 + slots,))],
        compiler_params=pltpu.CompilerParams(vmem_limit_bytes=1024 * 1024),
        name="write_out",
    )(*results)


def solution(mesh):
    in_specs = (
        P("ep", "dp", None),
        P("ep", "dp", None),
        P("ep", "dp"),
        P("ep", None, "dp"),
        P(None, "ep", "dp"),
        P(None, "ep", "dp"),
        P(None, "ep", "dp"),
        P(),
        P(),
    )
    out_specs = (
        P("ep", "dp", None),
        P("ep", "dp", None),
        P(None, "ep", "dp"),
        P(None, "ep", "dp"),
        P(None, "ep", "dp"),
        P("ep", None, "dp"),
    )
    step = functools.partial(local_step, mesh.shape["ep"], mesh.shape["dp"])
    return jax.shard_map(step, mesh=mesh, in_specs=in_specs, out_specs=out_specs, check_vma=False)
```

```python
import functools
import math

import jax
import jax.numpy as jnp
from jax import lax
from jax.experimental import pallas as pl
from jax.experimental.pallas import tpu as pltpu
from jax.sharding import PartitionSpec as P

STEP = 100
beta_one = 0.9
beta_two = 0.999
learn_rate = 0.02
epsilon = 1e-08
decay_rate = 0.1

MESH = pl.DeviceIdType.MESH


def adamw(master, moment_one, moment_two, expert_grad):
    first_new = beta_one * moment_one + (1.0 - beta_one) * expert_grad
    second_new = beta_two * moment_two + (1.0 - beta_two) * expert_grad * expert_grad
    first_hat = first_new / (1.0 - beta_one**STEP)
    second_hat = second_new / (1.0 - beta_two**STEP)
    updated = master - learn_rate * (
        first_hat / (jnp.sqrt(second_hat) + epsilon) + decay_rate * master
    )
    return (updated, first_new, second_new)


def split(x):
    high = x.astype(jnp.bfloat16)
    low = (x - high.astype(jnp.float32)).astype(jnp.bfloat16)
    return high, low


def dot3(a, b, dims):
    def one(p, q):
        return lax.dot_general(p, q, (dims, ((), ())), preferred_element_type=jnp.float32)

    return one(a[0], b[0]) + (one(a[0], b[1]) + one(a[1], b[0]))


VMEM_KIB = 52400


def piece_blocks(sides, slots, width):
    found = []
    for s in range(slots):
        for n in range(sides):
            cuts = [0, 128, width] if n == 0 and s == 0 and width % 128 == 0 and width > 128 else [0, width]
            found += [(n, s, low, high) for low, high in zip(cuts, cuts[1:])]
    return found


def kernel(nep, ndp, slots, *refs):
    old_hbm, new_hbm, counts_hbm, acts_hbm, grads_hbm, w_hbm, master_hbm, one_hbm, two_hbm = refs[:9]
    out_ref, ig_ref, nm_ref, no_ref, nt_ref = refs[9:14]
    ns_refs = refs[14:14 + slots]
    (
        acts_all, g_in, g_mask, g_send, g_cols, w_all, grad_send, arrived,
        master, one, two, pick_send, pick_recv, out_v, ig_v,
        old_ref, new_ref, counts_ref, table_sem, joined, opened,
        load_sem, store_sem,
        act_send_sem, act_recv_sem, w_send_sem, w_recv_sem, gs_sem, gr_sem,
        es_sem, er_sem, ps_sem, pr_sem,
    ) = refs[14 + slots:]
    ep = lax.axis_index("ep")
    dp = lax.axis_index("dp")
    half = ndp // 2
    sides, _, _, toks, width = acts_all.shape
    cols = w_all.shape[3]
    experts, rows, _ = master.shape
    _, chunks, _, crows, _ = grad_send.shape
    owners = nep // sides
    partner = dp + 1 - 2 * lax.rem(dp, 2)
    near = ep // owners
    quarter = ep // max(nep // 4, 1)
    outer = jnp.where((quarter == 0) | (quarter == 3), 0, 1)
    order = [lax.rem(near + outer + n, sides) for n in range(sides)]
    first = [jnp.where(side == near, 1, 0) for side in order]
    away = [lax.rem(near + 1 + n, sides) for n in range(sides)]
    skip = [0] * (sides - 1) + [1]
    place = lax.rem(ep, owners)

    def target(n_side, k):
        base = n_side * owners
        up = base + owners - 1 - k
        down = base + k
        other = jnp.where(n_side > near, up, down)
        mine = base + lax.rem(place + k, owners)
        return jnp.where(n_side == near, mine, other)

    def local(src, dst, sem):
        return pltpu.make_async_copy(src, dst, sem)

    def remote(src, dst, ssem, rsem, e, d):
        return pltpu.make_async_remote_copy(
            src_ref=src, dst_ref=dst, send_sem=ssem, recv_sem=rsem,
            device_id=(e, d), device_id_type=MESH)

    tables = [local(src, dst, table_sem.at[n]) for n, (src, dst) in
              enumerate(((counts_hbm, counts_ref), (old_hbm, old_ref), (new_hbm, new_ref)))]
    load_grads = [local(grads_hbm.at[s], g_in.at[s], load_sem.at[s]) for s in range(slots)]
    load_w = local(w_hbm, w_all.at[dp], load_sem.at[slots])
    load_opt = [local(src, dst, load_sem.at[slots + 1 + n]) for n, (src, dst) in
                enumerate(((master_hbm, master), (one_hbm, one), (two_hbm, two)))]
    pieces = [(n, s) for s in range(slots) for n in range(sides)]
    blocks = piece_blocks(sides, slots, width)

    def load_block(b):
        n, s, low, high = blocks[b]
        start = pl.multiple_of(away[n] * width + low, math.gcd(width, 128))
        return local(acts_hbm.at[s, :, pl.ds(start, high - low)], acts_all.at[away[n], dp, s, :, pl.ds(low, high - low)],
                     load_sem.at[slots + 4 + b])

    load_block(0).start()
    tables[0].start()
    load_grads[0].start()
    for b in range(1, len(blocks)):
        if blocks[b][:2] == pieces[0]:
            load_block(b).start()
    for c in load_grads[1:]:
        c.start()
    for b in range(1, len(blocks)):
        if blocks[b][:2] != pieces[0]:
            load_block(b).start()

    gate = ndp - 1
    barrier = pltpu.get_barrier_semaphore()
    for k in range(1, ndp):
        to = lax.rem(dp + k, ndp)

        @pl.when(to != gate)
        def _():
            pl.semaphore_signal(barrier, inc=1, device_id=(ep, to), device_id_type=MESH)

    @pl.when(dp != gate)
    def _():
        pl.semaphore_wait(barrier, ndp - 1)

    @pl.when(dp == gate - 1)
    def _():
        pl.semaphore_signal(joined, inc=1, device_id=(ep, gate), device_id_type=MESH)

    @pl.when(dp == gate)
    def _():
        pl.semaphore_wait(joined, 1)

        @pl.loop(1, nep)
        def _(k):
            pl.semaphore_signal(barrier, inc=1, device_id=(lax.rem(ep + k, nep), gate), device_id_type=MESH)

    def open_gate():
        @pl.when(dp == gate)
        def _():
            pl.semaphore_wait(barrier, nep - 1)
            for j in range(gate):
                pl.semaphore_signal(opened, inc=1, device_id=(ep, j), device_id_type=MESH)

    def pass_gate():
        @pl.when(dp != gate)
        def _():
            pl.semaphore_wait(opened, 1)

    def grad_copy(k, s):
        to = lax.rem(dp - k + ndp, ndp)
        return remote(g_send.at[to, s], g_cols.at[dp, s], gs_sem.at[k - 1, s], gr_sem.at[k - 1, s], ep, to)

    def grad_arrival(k, s):
        came = g_cols.at[lax.rem(dp + k, ndp), s]
        return remote(came, came, gs_sem.at[k - 1, s], gr_sem.at[k - 1, s], ep, partner)

    def block_copy(view, k, ssem, rsem):
        own = view(dp)
        to = partner if k == 0 else lax.rem(dp - 2 * k + ndp, ndp)
        return remote(own, own, ssem(k), rsem(k), ep, to)

    def block_arrival(view, k, ssem, rsem):
        if k == 0:
            came = view(partner)
        elif k < half:
            came = view(lax.rem(dp + 2 * k, ndp))
        else:
            came = view(lax.rem(partner + 2 * (k - half + 1), ndp))
        return remote(came, came, ssem(k), rsem(k), ep, partner)

    def block_relay(view, k, ssem, rsem):
        block = view(lax.rem(dp + 2 * k, ndp))
        return remote(block, block, ssem(half - 1 + k), rsem(half - 1 + k), ep, partner)

    def acts_kit(b):
        n, s, low, high = blocks[b]
        return (lambda i: acts_all.at[away[n], i, s, :, pl.ds(low, high - low)],
                lambda k: act_send_sem.at[k, b], lambda k: act_recv_sem.at[k, b])

    def w_kit(s):
        return (lambda i: w_all.at[i, s], lambda k: w_send_sem.at[k, s], lambda k: w_recv_sem.at[k, s])

    def send_block(view, ssem, rsem):
        for k in range(half - 1, -1, -1):
            block_copy(view, k, ssem, rsem).start()

    def relay_block(view, ssem, rsem):
        for k in range(1, half):
            block_arrival(view, k, ssem, rsem).wait_recv()
            block_relay(view, k, ssem, rsem).start()

    def finish_block(view, ssem, rsem):
        block_arrival(view, 0, ssem, rsem).wait_recv()
        for k in range(half, ndp - 1):
            block_arrival(view, k, ssem, rsem).wait_recv()

    load_block(0).wait()
    send_block(*acts_kit(0))
    tables[0].wait()
    for s in range(slots):
        load_grads[s].wait()
        live = (lax.broadcasted_iota(jnp.int32, (toks, 1), 0) < counts_ref[s]).astype(jnp.float32)
        masked = g_in[s] * live
        for j in range(ndp):
            g_send[j, s] = masked[:, j * cols:(j + 1) * cols]
        for k in range(ndp - 1, 0, -1):
            grad_copy(k, s).start()
        if s == 0:
            for b in range(1, len(blocks)):
                if blocks[b][:2] == pieces[0]:
                    load_block(b).wait()
                    send_block(*acts_kit(b))
            load_w.start()
            for c in tables[1:] + load_opt:
                c.start()
        g_mask[s] = masked
        g_cols[dp, s] = g_send[dp, s]
    for b in range(1, len(blocks)):
        if blocks[b][:2] != pieces[0]:
            load_block(b).wait()
            send_block(*acts_kit(b))
    load_w.wait()
    for s in range(slots):
        send_block(*w_kit(s))

    def send_grad(n, s, c):
        @pl.loop(skip[n], owners)
        def _(k):
            to = target(away[n], k)
            remote(grad_send.at[s, c, to], arrived.at[s, c, ep], es_sem.at[s, c], er_sem.at[s, c], to, dp).start()

    def send_some(n, s, start, stop):
        base = away[n] * owners

        @pl.loop(start, stop)
        def _(i):
            to = base + i

            @pl.when(to != ep)
            def _():
                for c in range(chunks):
                    remote(grad_send.at[s, c, to], arrived.at[s, c, ep], es_sem.at[s, c], er_sem.at[s, c], to, dp).start()

    seen, turned = set(), {}
    for b, (n, s, low, high) in enumerate(blocks):
        relay_block(*acts_kit(b))
        if b == 0:
            open_gate()
        finish_block(*acts_kit(b))
        left = split(acts_all[away[n], :, s, :, low:high].reshape(ndp * toks, high - low))
        if s not in seen:
            for k in range(1, ndp):
                grad_arrival(k, s).wait_recv()
            seen.add(s)
        if b == 0:
            grad = dot3(left, split(g_cols[:, s].reshape(ndp * toks, cols)), ((0,), (0,)))
        else:
            if s not in turned:
                turned[s] = split(g_cols[:, s].reshape(ndp * toks, cols).T)
            grad = dot3(turned[s], left, ((1,), (0,))).T
        base = away[n] * owners
        for i in range(owners):
            for c in range(chunks):
                at = i * rows + c * crows
                start, stop = max(at, low), min(at + crows, high)
                if start < stop:
                    grad_send[s, c, base + i, start - at:stop - at] = grad[start - low:stop - low]
        if b == 0:
            pass_gate()
        if (n, s) == pieces[0]:
            send_some(n, s, low // rows, high // rows)
        else:
            send_grad(n, s, 0)
    for c in range(1, chunks):
        for n, s in pieces[1:]:
            send_grad(n, s, c)
    for s in range(slots):
        for c in range(chunks):
            arrived[s, c, ep] = grad_send[s, c, ep]

    for c in tables[1:] + load_opt:
        c.wait()

    direct = rows % 8 == 0

    def landing(s, c, i):
        if direct:
            return ns_refs[s].at[pl.ds(pl.multiple_of(i * rows + c * crows, 8), crows)]
        return pick_recv.at[s, i]

    own_stores = []
    for c in range(chunks):
        for s in range(slots):
            came = arrived.at[s, c, pl.ds(0, nep - 1)]
            remote(came, came, es_sem.at[s, c], er_sem.at[s, c], ep, partner).wait_recv()
        span = slice(c * crows, (c + 1) * crows)

        @pl.loop(0, experts)
        def _(e):
            total = jnp.zeros((crows, cols), jnp.float32)
            for i in range(nep):
                for s in range(slots):
                    held = jnp.where(old_ref[i * slots + s] == e, 1.0, 0.0)
                    total = total + held * arrived[s, c, i]
            master[e, span], one[e, span], two[e, span] = adamw(
                master[e, span], one[e, span], two[e, span], total)

        def send_pick(to):
            for s in range(slots):
                pick_send[s, c, to] = master[new_ref[to * slots + s], span]
            for s in range(slots):
                remote(pick_send.at[s, c, to], landing(s, c, ep), ps_sem.at[s, c], pr_sem.at[s, c], to, dp).start()

        for n in range(sides):
            @pl.loop(first[n], owners)
            def _(k):
                send_pick(target(order[n], k))

        for s in range(slots):
            pick_send[s, c, ep] = master[new_ref[ep * slots + s], span]
            own_stores.append(local(pick_send.at[s, c, ep], landing(s, c, ep), store_sem.at[5 + s, c]))
            own_stores[-1].start()

    stores = [local(src, dst, store_sem.at[n, 0]) for n, (src, dst) in
              enumerate(((master, nm_ref), (one, no_ref), (two, nt_ref)))]
    for c in stores:
        c.start()

    for s in range(slots):
        relay_block(*w_kit(s))
    last = []
    for s in range(slots):
        finish_block(*w_kit(s))
        live = (lax.broadcasted_iota(jnp.int32, (toks, 1), 0) < counts_ref[s]).astype(jnp.float32)
        acts = [split(acts_all[h, dp, s] * live) for h in range(sides)]
        back = [jnp.zeros((toks, width), jnp.float32) for h in range(sides)]
        for j in range(ndp):
            at = slice(j * cols, (j + 1) * cols)
            grads = split(g_mask[s, :, at])
            total = jnp.zeros((toks, cols), jnp.float32)
            for h in range(sides):
                weights = split(w_all[j, s, h * width:(h + 1) * width])
                total = total + dot3(acts[h], weights, ((1,), (0,)))
                back[h] = back[h] + dot3(grads, weights, ((1,), (1,)))
            out_v[s, :, at] = total
        for h in range(sides):
            ig_v[s, :, h * width:(h + 1) * width] = back[h]
    last = [local(out_v, out_ref, store_sem.at[3, 0]), local(ig_v, ig_ref, store_sem.at[4, 0])]
    for c in last:
        c.start()

    for s in range(slots):
        for k in range(1, ndp):
            grad_copy(k, s).wait_send()
    for kit in [acts_kit(b) for b in range(len(blocks))] + [w_kit(s) for s in range(slots)]:
        for k in range(half):
            block_copy(kit[0], k, *kit[1:]).wait_send()
        for k in range(1, half):
            block_relay(kit[0], k, *kit[1:]).wait_send()
    for s in range(slots):
        for c in range(chunks):
            gone = grad_send.at[s, c, pl.ds(0, nep - 1)]
            remote(gone, gone, es_sem.at[s, c], er_sem.at[s, c], ep, partner).wait_send()
            gone = pick_send.at[s, c, pl.ds(0, nep - 1)]
            remote(gone, gone, ps_sem.at[s, c], pr_sem.at[s, c], ep, partner).wait_send()
    for c in own_stores + stores + last:
        c.wait()
    for s in range(slots):
        for c in range(chunks):
            if direct:
                came = ns_refs[s].at[pl.ds(0, (nep - 1) * crows)]
            else:
                came = pick_recv.at[s, pl.ds(0, nep - 1)]
            remote(came, came, ps_sem.at[s, c], pr_sem.at[s, c], ep, partner).wait_recv()
    if not direct:
        for s in range(slots):
            for i in range(nep):
                w_all[0, s, i * rows:(i + 1) * rows] = pick_recv[s, i]
            done = local(w_all.at[0, s], ns_refs[s], store_sem.at[0, 0])
            done.start()
            done.wait()


def write_out(slots, *refs):
    ins, outs, sems = refs[:5 + slots], refs[5 + slots:-1], refs[-1]
    parts = list(outs[:5]) + [outs[5].at[n] for n in range(slots)]
    copies = [pltpu.make_async_copy(src, dst, sems.at[n]) for n, (src, dst) in enumerate(zip(ins, parts))]
    for c in copies:
        c.start()
    for c in copies:
        c.wait()


def local_step(nep, ndp, activations, out_grads, counts, slot_weights, master, moment_one, moment_two, old_table, new_table):
    f32 = jnp.float32
    slots, toks, ff = activations.shape
    ds = out_grads.shape[2]
    cols = slot_weights.shape[2]
    experts, rows, _ = master.shape
    direct = rows % 8 == 0
    sides = 2
    chunks = 2 if rows % 16 == 0 else 1
    blocks = len(piece_blocks(sides, slots, ff // sides))
    parted = (slots, chunks, nep, rows // chunks, cols)
    hbm = pl.BlockSpec(memory_space=pl.ANY)
    dma = pltpu.SemaphoreType.DMA
    shapes = [
        jax.ShapeDtypeStruct(x.shape, f32)
        for x in (out_grads, activations, master, moment_one, moment_two, slot_weights)
    ]
    results = pl.pallas_call(
        functools.partial(kernel, nep, ndp, slots),
        out_shape=shapes[:5] + [jax.ShapeDtypeStruct((ff, cols), f32)] * slots,
        in_specs=[hbm] * 9,
        out_specs=[hbm] * (5 + slots),
        scratch_shapes=[
            pltpu.VMEM((sides, ndp, slots, toks, ff // sides), f32),
            pltpu.VMEM((slots, toks, ds), f32),
            pltpu.VMEM((slots, toks, ds), f32),
            pltpu.VMEM((ndp, slots, toks, cols), f32),
            pltpu.VMEM((ndp, slots, toks, cols), f32),
            pltpu.VMEM((ndp, slots, ff, cols), f32),
            pltpu.VMEM(parted, f32),
            pltpu.VMEM(parted, f32),
            pltpu.VMEM((experts, rows, cols), f32),
            pltpu.VMEM((experts, rows, cols), f32),
            pltpu.VMEM((experts, rows, cols), f32),
            pltpu.VMEM(parted, f32),
            pltpu.VMEM((1, 1, 8, 128) if direct else (slots, nep, rows, cols), f32),
            pltpu.VMEM((slots, toks, ds), f32),
            pltpu.VMEM((slots, toks, ff), f32),
            pltpu.SMEM((nep * slots,), jnp.int32),
            pltpu.SMEM((nep * slots,), jnp.int32),
            pltpu.SMEM((slots,), jnp.int32),
            dma((3,)),
            pltpu.SemaphoreType.REGULAR,
            pltpu.SemaphoreType.REGULAR,
            dma((slots + 4 + blocks,)),
            dma((5 + slots, chunks)),
            dma((ndp - 1, blocks)),
            dma((ndp - 1, blocks)),
            dma((ndp - 1, slots)),
            dma((ndp - 1, slots)),
            dma((ndp - 1, slots)),
            dma((ndp - 1, slots)),
            dma((slots, chunks)),
            dma((slots, chunks)),
            dma((slots, chunks)),
            dma((slots, chunks)),
        ],
        compiler_params=pltpu.CompilerParams(
            collective_id=0, has_side_effects=True, vmem_limit_bytes=VMEM_KIB * 1024
        ),
        name="step",
    )(*[pltpu.with_memory_space_constraint(x, pltpu.HBM) for x in (
        old_table.reshape(-1), new_table.reshape(-1), counts.reshape(-1),
        activations, out_grads, slot_weights, master, moment_one, moment_two)])
    return pl.pallas_call(
        functools.partial(write_out, slots),
        out_shape=shapes,
        in_specs=[hbm] * (5 + slots),
        out_specs=[hbm] * 6,
        scratch_shapes=[dma((5 + slots,))],
        compiler_params=pltpu.CompilerParams(vmem_limit_bytes=1024 * 1024),
        name="write_out",
    )(*results)


def solution(mesh):
    in_specs = (
        P("ep", "dp", None),
        P("ep", "dp", None),
        P("ep", "dp"),
        P("ep", None, "dp"),
        P(None, "ep", "dp"),
        P(None, "ep", "dp"),
        P(None, "ep", "dp"),
        P(),
        P(),
    )
    out_specs = (
        P("ep", "dp", None),
        P("ep", "dp", None),
        P(None, "ep", "dp"),
        P(None, "ep", "dp"),
        P(None, "ep", "dp"),
        P("ep", None, "dp"),
    )
    step = functools.partial(local_step, mesh.shape["ep"], mesh.shape["dp"])
    return jax.shard_map(step, mesh=mesh, in_specs=in_specs, out_specs=out_specs, check_vma=False)
```
